32 devices in a mesh: fsdp: 4 (over z), tp: 8 (over y, x, core).
Axes of the slice: x: 2, y: 2, z: 4, core: 2. Of those that a mesh axis runs over, the one named last changes fastest.
Arguments:
- tokens: bfloat16 [3008, 4096], P('fsdp', 'tp'), may hold values from -6 to 6
- norm_gain: float32 [4096], replicated, may hold values from 0.5 to 1.5
- base_gate: bfloat16 [4096, 12288], P(None, 'tp'), may hold values from -0.09375 to 0.09375
- base_up: bfloat16 [4096, 12288], P(None, 'tp'), may hold values from -0.09375 to 0.09375
- base_down: bfloat16 [12288, 4096], P('tp'), may hold values from -0.0546875 to 0.0546875
- code_gate: bfloat16 [4096, 12288], P(('fsdp', 'tp')), may hold values from -4 to 4
- code_up: bfloat16 [4096, 12288], P(('fsdp', 'tp')), may hold values from -4 to 4
- scale_gate: float32 [4096, 96], P(('fsdp', 'tp')), may hold values from 0.005 to 0.05
- scale_up: float32 [4096, 96], P(('fsdp', 'tp')), may hold values from 0.005 to 0.05
- code_down: bfloat16 [12288, 4096], P(None, ('fsdp', 'tp')), may hold values from -4 to 4
- scale_down: float32 [96, 4096], P(None, ('fsdp', 'tp')), may hold values from 0.005 to 0.05
- cu_seqlens: int32 [4, 9], P('fsdp'), may hold values from 0 to 752, as said below
Outputs:
- mixed: bfloat16 [3008, 4096], P('fsdp', 'tp')
- seq_means: float32 [32, 4096], P('fsdp', 'tp')
The draws below stay inside these ranges and needn't reach their ends.
Inputs may be any that keep to these rules, and one draw needn't show every extreme that they name: `cu_seqlens`: each row starts at 0 and rises strictly; its last entry is the group's live tokens, which fill the first slots of its 752. Over all groups the live tokens add up to exactly 1536, and some group has exactly 752.
All inputs are finite; a program needn't handle non-finite values.
Results may differ from the reference program's by a relative error of at most 0.023.
Values may be sent and summed in bfloat16 or wider, within the bound.
A program may use at most 256 MiB of HBM per device.

```python
import math
import jax
import jax.numpy as jnp
from jax import lax

D = 4096
FF = 12288
BLK = 128
SEQS = 8
BAL = 384
CAP = 752
GROUPS = 4
TOKENS = 3008
N_TP = 8


def draw_cu_seqlens(key, part):
    key_pairs = jax.random.fold_in(key, 11)
    key_order = jax.random.fold_in(key, 12)
    key_cuts = jax.random.fold_in(key, 13)
    spread = jax.random.randint(key_pairs, (GROUPS // 2,), 0, BAL - 2 * SEQS + 1).astype(jnp.int32)
    spread = spread.at[0].set(BAL - 2 * SEQS)
    counts = jnp.stack([BAL + spread, BAL - spread], axis=1).reshape(GROUPS)
    counts = counts[jax.random.permutation(key_order, GROUPS)]
    upper_bound = (counts - SEQS + 1)[:, None]
    cut_points = jax.random.randint(key_cuts, (GROUPS, SEQS - 1), 0, upper_bound).astype(jnp.int32)
    cut_points = jnp.sort(cut_points, axis=1) + jnp.arange(1, SEQS, dtype=jnp.int32)[None, :]
    leading = jnp.zeros((GROUPS, 1), jnp.int32)
    return jnp.concatenate([leading, cut_points, counts[:, None].astype(jnp.int32)], axis=1)


def levels(key, dims, cuts, low, high):
    def one(axis_at, shards_of):
        steps = jax.random.uniform(jax.random.fold_in(jax.random.fold_in(key, 6), axis_at), (shards_of,), jnp.float32, low / len(cuts), high / len(cuts))
        return jnp.repeat(jnp.exp(steps), dims[axis_at] // shards_of).reshape((-1,) + (1,) * (len(dims) - axis_at - 1))

    factor_of = one(*cuts[0])
    for cut in cuts[1:]:
        factor_of = factor_of * one(*cut)
    return factor_of


def gaussian(key, dims, width, reach, shards=(), kind=jnp.bfloat16):
    values = jax.random.normal(key, dims, jnp.float32) * width
    if len(shards) > 0:
        values = levels(key, dims, shards, -0.22, 0.18) * values
    return jnp.clip(values, min=-reach, max=reach).astype(kind)


def setup_inputs(seed: int = 0) -> dict:
    seeds = jax.random.split(jax.random.key(seed), 13)
    tokens = gaussian(seeds[0], (TOKENS, D), 1.0, 6.0, ((0, 4), (1, 8)))
    norm_gain = jnp.clip(jax.random.uniform(seeds[1], (D,), jnp.float32, 0.5, 1.5), 0.5, 1.5)
    base_gate = gaussian(seeds[2], (D, FF), D ** -0.5, 0.09375, ((1, 8),))
    base_up = gaussian(seeds[3], (D, FF), D ** -0.5, 0.09375, ((1, 8),))
    base_down = gaussian(seeds[4], (FF, D), FF ** -0.5, 0.0546875, ((0, 8),))
    code_gate = gaussian(seeds[5], (D, FF), 1.0, 4.0, ((0, 32),))
    code_up = gaussian(seeds[6], (D, FF), 1.0, 4.0, ((0, 32),))
    scale_gate = jnp.clip(jnp.exp(math.log(0.05) - 2.3025851 * jax.random.uniform(seeds[7], (D, FF // BLK), jnp.float32) ** levels(seeds[7], (D, FF // BLK), ((0, 32),), -0.2, 0.2)), 0.005, 0.05)
    scale_up = jnp.clip(jnp.exp(math.log(0.05) - 2.3025851 * jax.random.uniform(seeds[8], (D, FF // BLK), jnp.float32) ** levels(seeds[8], (D, FF // BLK), ((0, 32),), -0.2, 0.2)), 0.005, 0.05)
    code_down = gaussian(seeds[9], (FF, D), 1.0, 4.0, ((1, 32),))
    scale_down = jnp.clip(jnp.exp(math.log(0.05) - 2.3025851 * jax.random.uniform(seeds[10], (FF // BLK, D), jnp.float32) ** levels(seeds[10], (FF // BLK, D), ((1, 32),), -0.2, 0.2)), 0.005, 0.05)
    cu_seqlens = draw_cu_seqlens(jax.random.fold_in(seeds[12], 71), 0)
    return {"tokens": tokens, "norm_gain": norm_gain, "base_gate": base_gate, "base_up": base_up, "base_down": base_down, "code_gate": code_gate, "code_up": code_up, "scale_gate": scale_gate, "scale_up": scale_up, "code_down": code_down, "scale_down": scale_down, "cu_seqlens": cu_seqlens}


EPSILON = 1e-06

def reference(tokens, norm_gain, base_gate, base_up, base_down, code_gate, code_up, scale_gate, scale_up, code_down, scale_down, cu_seqlens):
    w_gate = (base_gate.astype(jnp.float32) + code_gate.astype(jnp.float32) * jnp.repeat(scale_gate, BLK, axis=1)).astype(jnp.bfloat16)
    w_up = (base_up.astype(jnp.float32) + code_up.astype(jnp.float32) * jnp.repeat(scale_up, BLK, axis=1)).astype(jnp.bfloat16)
    w_down = (base_down.astype(jnp.float32) + code_down.astype(jnp.float32) * jnp.repeat(scale_down, BLK, axis=0)).astype(jnp.bfloat16)
    slice_width = FF // N_TP
    down_slices = w_down.reshape(N_TP, slice_width, D)
    stacked = tokens.reshape(GROUPS, CAP, D)
    positions = jnp.arange(CAP, dtype=jnp.int32)

    def one_group(operands):
        rows_in, bounds = operands
        widened = rows_in.astype(jnp.float32)
        inverse = lax.rsqrt(lax.optimization_barrier(jnp.mean(widened * widened, axis=1, keepdims=True)) + EPSILON)
        normed = (widened * inverse * norm_gain[None, :]).astype(jnp.bfloat16)
        gate_out = jnp.dot(normed, w_gate, preferred_element_type=jnp.float32)
        up_out = jnp.dot(normed, w_up, preferred_element_type=jnp.float32)
        hidden = (jax.nn.silu(gate_out) * up_out).astype(jnp.bfloat16)
        hidden_slices = hidden.reshape(CAP, N_TP, slice_width).transpose(1, 0, 2)

        def add_slice(running, pair):
            partial_value = jnp.dot(pair[0], pair[1], preferred_element_type=jnp.float32).astype(jnp.bfloat16)
            return (running + partial_value.astype(jnp.float32), None)
        summed, _ = lax.scan(add_slice, jnp.zeros((CAP, D), jnp.float32), (hidden_slices, down_slices))
        mixed_rows = (widened + summed).astype(jnp.bfloat16)
        live_count = bounds[SEQS]
        mixed_rows = jnp.where((positions < live_count)[:, None], mixed_rows, jnp.zeros((), jnp.bfloat16))
        member = (positions[None, :] >= bounds[:-1, None]) & (positions[None, :] < bounds[1:, None])
        seq_sums = jnp.dot(member.astype(jnp.bfloat16), mixed_rows, preferred_element_type=jnp.float32)
        lengths = (bounds[1:] - bounds[:-1]).astype(jnp.float32)
        return (mixed_rows, seq_sums / lengths[:, None])
    mixed_all, means_all = lax.map(one_group, (stacked, cu_seqlens))
    return (mixed_all.reshape(GROUPS * CAP, D), means_all.reshape(GROUPS * SEQS, D))
```

```python
import functools
import jax
import jax.numpy as jnp
from jax import lax
from jax.experimental import pallas as pl
from jax.experimental.pallas import tpu as pltpu
from jax.sharding import PartitionSpec as P

SEQS = 8
EPSILON = 1e-06
BLOCKS = 2
F32, BF16 = jnp.float32, jnp.bfloat16
MESH = pl.DeviceIdType.MESH


def al(value, size):
    return pl.multiple_of(value, size)


def layer_kernel(n, m, down_here, *refs):
    (x_ref, cg_in, cu_in, st_ref, bg_in, bu_in, cd_in, sd_ref, bd_in, out_ref,
     cg, cu, base, own, got, hid, cd, bd,
     s_code, r_code, s_down, r_down, l_sem, b_sem, s_red, r_red, s_hid, r_hid) = refs
    f, t = lax.axis_index("fsdp"), lax.axis_index("tp")
    kr = cg_in.shape[0]
    depth, units = cg.shape
    cw = base.shape[3]
    chunks = units // cw
    rows = x_ref.shape[0] // BLOCKS
    half = rows // 2
    total = BLOCKS * chunks
    last = n - 1

    barrier = pltpu.get_barrier_semaphore()
    for d in range(1, m):
        pl.semaphore_signal(barrier, inc=1, device_id={"tp": lax.rem(t + d, m)}, device_id_type=MESH)
    for d in range(1, n):
        pl.semaphore_signal(barrier, inc=1, device_id={"fsdp": lax.rem(f + d, n)}, device_id_type=MESH)

    def base_copy(c, slot, which, src):
        return pltpu.make_async_copy(
            src.at[pl.ds(al(f * depth, 16), depth), pl.ds(al(c * cw, 128), cw)],
            base.at[slot, which], b_sem.at[slot, which])

    def base_start(c, slot):
        base_copy(c, slot, 0, bg_in).start()
        base_copy(c, slot, 1, bu_in).start()

    mine = pl.ds(al(t * kr, 16), kr)
    cols = pl.ds(al(t * units, 128), units)
    local = [pltpu.make_async_copy(cg_in.at[:, cols], cg.at[mine, :], l_sem.at[0]),
             pltpu.make_async_copy(cu_in.at[:, cols], cu.at[mine, :], l_sem.at[1]),
             pltpu.make_async_copy(bd_in.at[:, pl.ds(al(f * depth, 128), depth)], bd, l_sem.at[2])]
    if down_here:
        dcw = cd_in.shape[1]
        local.append(pltpu.make_async_copy(
            cd_in.at[pl.ds(al(t * units, 16), units), :], cd.at[:, pl.ds(al(t * dcw, 128), dcw)], l_sem.at[3]))
    else:
        local.append(pltpu.make_async_copy(cd_in, cd, l_sem.at[3]))
    base_start(0, 0)
    for copy in local:
        copy.start()
    pl.semaphore_wait(barrier, m + n - 2)

    def code_copy(c, which, d):
        src, dst = ((cg_in, cg), (cu_in, cu))[which]
        to = lax.rem(t + d, m)
        return pltpu.make_async_remote_copy(
            src_ref=src.at[:, pl.ds(al(to * units + c * cw, 128), cw)],
            dst_ref=dst.at[mine, pl.ds(al(c * cw, 128), cw)],
            send_sem=s_code.at[c, which, d], recv_sem=r_code.at[c, which, d],
            device_id={"tp": to}, device_id_type=MESH)

    def down_copy(d):
        to = lax.rem(t + d, m)
        return pltpu.make_async_remote_copy(
            src_ref=cd_in.at[pl.ds(al(to * units, 16), units), :],
            dst_ref=cd.at[:, pl.ds(al(t * dcw, 128), dcw)],
            send_sem=s_down.at[d], recv_sem=r_down.at[d],
            device_id={"tp": to}, device_id_type=MESH)

    @pl.loop(0, chunks)
    def _(c):
        for d in range(1, m):
            code_copy(c, 0, d).start()
            code_copy(c, 1, d).start()

    if down_here:
        for d in range(1, m):
            down_copy(d).start()
    local[0].wait()
    local[1].wait()

    def unpack(c):
        slot = lax.rem(c, 2)

        @pl.when(c + 1 < chunks)
        def _():
            base_start(c + 1, 1 - slot)
        base_copy(c, slot, 0, bg_in).wait()
        base_copy(c, slot, 1, bu_in).wait()
        for d in range(1, m):
            code_copy(c, 0, d).wait_recv()
            code_copy(c, 1, d).wait_recv()
        here = pl.ds(al(c * cw, 128), cw)
        scales = st_ref[...]
        lane = lax.broadcasted_iota(jnp.int32, scales.shape, 1)
        for which, codes in ((0, cg), (1, cu)):
            picked = jnp.where(lane == c + which * chunks, scales, 0.0)
            column = jnp.sum(picked, axis=1, keepdims=True)
            codes[:, here] = (base[slot, which].astype(F32) + codes[:, here].astype(F32) * column).astype(BF16)

    def partial(k):
        b, c = k // chunks, lax.rem(k, chunks)

        @pl.when(b == 0)
        def _():
            unpack(c)
        here = pl.ds(al(c * cw, 128), cw)
        both = jnp.concatenate([cg[:, here], cu[:, here]], axis=1)
        for side in range(2):
            xs = x_ref[pl.ds(al(b * rows + side * half, 16), half), :]
            own[side, k] = jnp.dot(xs, both, preferred_element_type=F32).astype(BF16)

    def spot(k, side):
        b, c = k // chunks, lax.rem(k, chunks)
        return hid.at[pl.ds(al(b * rows + side * half, 16), half), pl.ds(al(c * cw, 128), cw)]

    def red_copy(k, side):
        return pltpu.make_async_remote_copy(
            src_ref=own.at[side, k], dst_ref=got.at[side, k], send_sem=s_red.at[side, k], recv_sem=r_red.at[side, k],
            device_id={"fsdp": jnp.clip(f + (1 if side else -1), 0, last)}, device_id_type=MESH)

    def hid_copy(k, side):
        return pltpu.make_async_remote_copy(
            src_ref=spot(k, side), dst_ref=spot(k, side), send_sem=s_hid.at[side, k], recv_sem=r_hid.at[side, k],
            device_id={"fsdp": jnp.clip(f + (-1 if side else 1), 0, last)}, device_id_type=MESH)

    def valid(k):
        return (k >= 0) & (k < total)

    def reduce_step(s, side):
        far = f if side else last - f
        k = s - far

        @pl.when(valid(k) & (far > 0))
        def _():
            red_copy(k, side).wait_recv()

            @pl.when(far < last)
            def _():
                own[side, k] = (own[side, k].astype(F32) + got[side, k].astype(F32)).astype(BF16)

            @pl.when(far == last)
            def _():
                both = own[side, k].astype(F32) + got[side, k].astype(F32)
                gate, up = both[:, :cw], both[:, cw:]
                b, c = k // chunks, lax.rem(k, chunks)
                hid[pl.ds(al(b * rows + side * half, 16), half), pl.ds(al(c * cw, 128), cw)] = (
                    jax.nn.silu(gate) * up).astype(BF16)

    def reduce_send(s, side):
        far = f if side else last - f
        k = s - far

        @pl.when(valid(k) & (far < last))
        def _():
            red_copy(k, side).start()

        @pl.when(valid(k) & (far == last))
        def _():
            hid_copy(k, side).start()

    def pass_on(s, side):
        far = f if side else last - f
        k = s - last - (last - far)

        @pl.when(valid(k) & (far < last))
        def _():
            hid_copy(k, side).wait_recv()

            @pl.when(far > 0)
            def _():
                hid_copy(k, side).start()

    partial(0)

    @pl.loop(0, total + 2 * last)
    def _(s):
        for side in range(2):
            reduce_step(s, side)
        for side in range(2):
            reduce_send(s, side)
        for side in range(2):
            pass_on(s, side)

        @pl.when(s + 1 < total)
        def _():
            partial(s + 1)
        done = s - 2 * last

        @pl.when(done == chunks - 1)
        def _():
            local[2].wait()
            local[3].wait()
            if down_here:
                for d in range(1, m):
                    down_copy(d).wait_recv()

            @pl.loop(0, chunks)
            def _(c):
                there = pl.ds(al(c * cw, 16), cw)
                cd[there, :] = (bd[there, :].astype(F32) + cd[there, :].astype(F32) * sd_ref[c]).astype(BF16)

        @pl.when((done >= 0) & (lax.rem(done, chunks) == chunks - 1))
        def _():
            b = done // chunks

            @pl.loop(0, 2)
            def _(side):
                part = pl.ds(al(b * rows + side * half, 16), half)
                out_ref[part, :] = jnp.dot(hid[part, :], cd[...], preferred_element_type=F32).astype(BF16)

    @pl.loop(0, chunks)
    def _(c):
        for d in range(1, m):
            code_copy(c, 0, d).wait_send()
            code_copy(c, 1, d).wait_send()
    if down_here:
        for d in range(1, m):
            down_copy(d).wait_send()

    @pl.loop(0, total)
    def _(k):
        for side in range(2):
            far = f if side else last - f

            @pl.when(far < last)
            def _():
                red_copy(k, side).wait_send()

            @pl.when(far > 0)
            def _():
                hid_copy(k, side).wait_send()


def layer(n, m, x, code_gate, code_up, st, base_gate, base_up, code_down, sd, base_down, down_here):
    rows, depth = x.shape
    units = base_gate.shape[1]
    cw = code_gate.shape[1] // (sd.shape[0] * m)
    chunks = units // cw
    total = BLOCKS * chunks
    half = rows // (2 * BLOCKS)
    anywhere = pl.BlockSpec(memory_space=pl.ANY)
    near = pl.BlockSpec(memory_space=pltpu.VMEM)
    dma = pltpu.SemaphoreType.DMA
    return pl.pallas_call(
        functools.partial(layer_kernel, n, m, down_here),
        out_shape=jax.ShapeDtypeStruct((rows, depth), BF16),
        in_specs=[near, anywhere, anywhere, near, anywhere, anywhere, anywhere, near, anywhere],
        out_specs=near,
        scratch_shapes=[
            pltpu.VMEM((depth, units), BF16), pltpu.VMEM((depth, units), BF16),
            pltpu.VMEM((2, 2, depth, cw), BF16),
            pltpu.VMEM((2, total, half, 2 * cw), BF16), pltpu.VMEM((2, total, half, 2 * cw), BF16),
            pltpu.VMEM((rows, units), BF16),
            pltpu.VMEM((units, depth), BF16), pltpu.VMEM((units, depth), BF16),
            dma((chunks, 2, m)), dma((chunks, 2, m)), dma((m,)), dma((m,)), dma((4,)), dma((2, 2)),
            dma((2, total)), dma((2, total)), dma((2, total)), dma((2, total)),
        ],
        compiler_params=pltpu.CompilerParams(
            collective_id=0, has_side_effects=True, vmem_limit_bytes=67043328),
    )(x, code_gate, code_up, st, base_gate, base_up, code_down, sd, base_down)


def shards(tokens, norm_gain, base_gate, base_up, base_down, code_gate, code_up,
           scale_gate, scale_up, code_down, scale_down, cu_seqlens):
    n, m = lax.axis_size("fsdp"), lax.axis_size("tp")
    me_f, me_t = lax.axis_index("fsdp"), lax.axis_index("tp")
    cap, feat = tokens.shape
    width, units = base_gate.shape
    depth = width // n
    live_all = n * (cap // 2 + SEQS)
    lanes = BLOCKS * m
    rp = live_all // lanes
    ns = -(-(-(-cap // lanes)) // 16) * 16
    kr = code_gate.shape[0]
    nb = scale_gate.shape[1] // m

    bounds_all = lax.all_gather(cu_seqlens, "fsdp", axis=0, tiled=True)
    counts = bounds_all[:, SEQS]
    starts = jnp.cumsum(counts) - counts
    start, live = starts[me_f], counts[me_f]

    q_of = (jnp.arange(m)[:, None] + m * jnp.arange(BLOCKS)[None, :])
    row_of = ((q_of - start) % lanes)[:, :, None] + lanes * jnp.arange(ns)[None, None, :]
    row_of = jnp.where(row_of < live, row_of, -1).reshape(-1)
    slots = jnp.arange(cap, dtype=jnp.int32)
    spread = (row_of[:, None] == slots[None, :]).astype(BF16)
    sent = jnp.dot(spread, tokens, preferred_element_type=F32).astype(BF16)
    wide = lax.all_to_all(sent.reshape(m, BLOCKS * ns, feat), "tp", split_axis=0, concat_axis=0, tiled=True)
    wide = wide.transpose(1, 0, 2).reshape(BLOCKS * ns, width).astype(F32)
    inverse = lax.rsqrt(jnp.mean(wide * wide, axis=1, keepdims=True) + EPSILON)
    normed = (wide * inverse * norm_gain[None, :]).astype(BF16)
    block = lax.all_to_all(normed.reshape(BLOCKS * ns, n, depth), "fsdp", split_axis=1, concat_axis=1, tiled=True)

    q_mine = me_t + m * jnp.arange(BLOCKS)
    r_all = ((q_mine[:, None] - starts[None, :]) % lanes)[:, :, None] + lanes * jnp.arange(ns)[None, None, :]
    slot_all = jnp.where(r_all < counts[None, :, None], (starts[None, :, None] + r_all) // lanes, -1)
    by_group = block.reshape(BLOCKS, ns, n, depth).transpose(0, 2, 1, 3).reshape(BLOCKS, n * ns, depth)
    place = (slot_all.reshape(BLOCKS, 1, n * ns) == jnp.arange(rp)[None, :, None]).astype(BF16)
    mine = jnp.einsum("brk,bkd->brd", place, by_group, preferred_element_type=F32).astype(BF16)
    x = lax.all_gather(mine, "tp", axis=1, tiled=True).reshape(live_all, depth)

    both = jnp.stack([scale_gate.reshape(kr, m, nb), scale_up.reshape(kr, m, nb)], axis=2).reshape(kr, m * 2 * nb)
    st = lax.all_to_all(both, "tp", split_axis=1, concat_axis=0, tiled=True)
    st = jnp.pad(st, ((0, 0), (0, -(2 * nb) % 128)))
    sd = lax.all_to_all(scale_down, "tp", split_axis=0, concat_axis=1, tiled=True)[:, None, :]
    down_here = code_down.shape[1] % 128 == 0
    if not down_here:
        code_down = lax.all_to_all(code_down, "tp", split_axis=0, concat_axis=1, tiled=True)
    out_part = layer(n, m, x, code_gate, code_up, st, base_gate, base_up, code_down, sd, base_down, down_here)

    summed = lax.psum_scatter(out_part.reshape(BLOCKS, m * rp, depth), "tp", scatter_dimension=1, tiled=True)
    back = jnp.einsum("brk,brd->bkd", place, summed, preferred_element_type=F32).astype(BF16)
    back = back.reshape(BLOCKS, n, ns, depth).transpose(1, 0, 2, 3).reshape(n, BLOCKS * ns, depth)
    back = lax.all_to_all(back, "fsdp", split_axis=0, concat_axis=0, tiled=True)
    back = back.transpose(1, 0, 2).reshape(BLOCKS * ns, m, feat).transpose(1, 0, 2)
    back = lax.all_to_all(back, "tp", split_axis=0, concat_axis=0, tiled=True).reshape(m * BLOCKS * ns, feat)
    summed_out = lax.dot_general(spread, back, (((0,), (0,)), ((), ())), preferred_element_type=F32)

    bounds = cu_seqlens[0]
    mixed = (tokens.astype(F32) + summed_out).astype(BF16)
    mixed = jnp.where((slots < live)[:, None], mixed, jnp.zeros((), BF16))
    member = (slots[None, :] >= bounds[:-1, None]) & (slots[None, :] < bounds[1:, None])
    seq_sums = jnp.dot(member.astype(BF16), mixed, preferred_element_type=F32)
    lengths = (bounds[1:] - bounds[:-1]).astype(F32)
    return mixed, seq_sums / lengths[:, None]


def solution(mesh):
    placed = (
        P("fsdp", "tp"), P(), P(None, "tp"), P(None, "tp"), P("tp", None),
        P(("fsdp", "tp"), None), P(("fsdp", "tp"), None),
        P(("fsdp", "tp"), None), P(("fsdp", "tp"), None),
        P(None, ("fsdp", "tp")), P(None, ("fsdp", "tp")), P("fsdp", None),
    )
    return jax.shard_map(shards, mesh=mesh, in_specs=placed,
                         out_specs=(P("fsdp", "tp"), P("fsdp", "tp")), check_vma=False)
```

```python
import functools
import jax
import jax.numpy as jnp
from jax import lax
from jax.experimental import pallas as pl
from jax.experimental.pallas import tpu as pltpu
from jax.sharding import PartitionSpec as P

SEQS = 8
EPSILON = 1e-06
BLOCKS = 2
F32, BF16 = jnp.float32, jnp.bfloat16
MESH = pl.DeviceIdType.MESH


def al(value, size):
    return pl.multiple_of(value, size)


def layer_kernel(n, m, here, *refs):
    (sent, gain_ref, row_ref, col_ref, cg_in, cu_in, sg_in, bg_in, bu_in, cd_in, sd_in, bd_in, out_ref,
     cg, cu, base, own, got, hid, cd, bd, x_ref, wide, cut, grp, part_out, part_in, back, back_wide, st, sct, sd,
     s_code, r_code, s_down, r_down, l_sem, b_sem, s_red, r_red, s_hid, r_hid,
     s_tp, r_tp, s_fs, r_fs, s_sc, r_sc) = refs
    f, t = lax.axis_index("fsdp"), lax.axis_index("tp")
    kr = cg_in.shape[0]
    depth, units = cg.shape
    cw = base.shape[3]
    chunks = units // cw
    rows = x_ref.shape[0] // BLOCKS
    half = rows // 2
    rp = rows // m
    ns, feat = sent.shape[2], sent.shape[3]
    nb2 = sg_in.shape[-2]
    total = BLOCKS * chunks
    last = n - 1
    dcw = depth // m

    barrier = pltpu.get_barrier_semaphore()
    for d in range(1, m):
        pl.semaphore_signal(barrier, inc=1, device_id={"tp": lax.rem(t + d, m)}, device_id_type=MESH)
    for d in range(1, n):
        pl.semaphore_signal(barrier, inc=1, device_id={"fsdp": lax.rem(f + d, n)}, device_id_type=MESH)

    def base_copy(c, slot, which, src):
        return pltpu.make_async_copy(
            src.at[pl.ds(al(f * depth, 16), depth), pl.ds(al(c * cw, 128), cw)],
            base.at[slot, which], b_sem.at[slot, which])

    def base_start(c, slot):
        base_copy(c, slot, 0, bg_in).start()
        base_copy(c, slot, 1, bu_in).start()

    mine = pl.ds(al(t * kr, 16), kr)
    cols = pl.ds(al(t * units, 128), units)
    local = [pltpu.make_async_copy(cg_in.at[:, cols], cg.at[mine, :], l_sem.at[0]),
             pltpu.make_async_copy(cu_in.at[:, cols], cu.at[mine, :], l_sem.at[1]),
             pltpu.make_async_copy(bd_in.at[:, pl.ds(al(f * depth, 128), depth)], bd, l_sem.at[2])]
    if here:
        local += [pltpu.make_async_copy(
            cd_in.at[pl.ds(al(t * units, 16), units), :], cd.at[:, pl.ds(al(t * dcw, 128), dcw)], l_sem.at[3]),
            pltpu.make_async_copy(sd_in.at[t], sd.at[:, pl.ds(al(t * dcw, 128), dcw)], l_sem.at[4]),
            pltpu.make_async_copy(sg_in.at[t], sct.at[0:nb2, pl.ds(al(t * kr, 128), kr)], l_sem.at[5])]
    else:
        local += [pltpu.make_async_copy(cd_in, cd, l_sem.at[3]), pltpu.make_async_copy(sd_in, sd, l_sem.at[4]),
                  pltpu.make_async_copy(sg_in, sct.at[0:nb2, :], l_sem.at[5])]
    base_start(0, 0)
    if nb2 < sct.shape[0]:
        sct[nb2:, :] = jnp.zeros_like(sct[nb2:, :])
    for copy in local:
        copy.start()

    def to_tp(b, stage, d, src, dst):
        return pltpu.make_async_remote_copy(
            src_ref=src, dst_ref=dst, send_sem=s_tp.at[stage, b, d], recv_sem=r_tp.at[stage, b, d],
            device_id={"tp": lax.rem(t + d, m)}, device_id_type=MESH)

    def to_fs(b, stage, d, src, dst):
        return pltpu.make_async_remote_copy(
            src_ref=src, dst_ref=dst, send_sem=s_fs.at[stage, b, d], recv_sem=r_fs.at[stage, b, d],
            device_id={"fsdp": lax.rem(f + d, n)}, device_id_type=MESH)

    my_feat = pl.ds(al(t * feat, 128), feat)
    my_depth = pl.ds(al(f * depth, 128), depth)

    def my_part(b):
        return pl.ds(al(b * rows + t * rp, 16), rp)

    def rows_out(b, d):
        return to_tp(b, 0, d, sent.at[lax.rem(t + d, m), b], wide.at[b, :, my_feat])

    def normed_out(b, d):
        return to_fs(b, 0, d, cut.at[b, lax.rem(f + d, n)], grp.at[b, pl.ds(al(f * ns, 16), ns), :])

    def x_out(b, d):
        return to_tp(b, 1, d, x_ref.at[my_part(b), :], x_ref.at[my_part(b), :])

    def sum_out(b, d):
        return to_tp(b, 2, d, part_out.at[b, lax.rem(t + d, m)], part_in.at[b, t])

    def back_out(b, d):
        return to_fs(b, 1, d, back.at[b, lax.rem(f + d, n)], back_wide.at[b, :, my_depth])

    def home_out(b, d):
        return to_tp(b, 3, d, back_wide.at[b, :, pl.ds(al(lax.rem(t + d, m) * feat, 128), feat)], out_ref.at[t, b])

    def scale_copy(d):
        to = lax.rem(t + d, m)
        return pltpu.make_async_remote_copy(
            src_ref=sg_in.at[to], dst_ref=sct.at[0:nb2, pl.ds(al(t * kr, 128), kr)],
            send_sem=s_sc.at[0, d], recv_sem=r_sc.at[0, d], device_id={"tp": to}, device_id_type=MESH)

    def scale_down_copy(d):
        to = lax.rem(t + d, m)
        return pltpu.make_async_remote_copy(
            src_ref=sd_in.at[to], dst_ref=sd.at[:, pl.ds(al(t * dcw, 128), dcw)],
            send_sem=s_sc.at[1, d], recv_sem=r_sc.at[1, d], device_id={"tp": to}, device_id_type=MESH)

    def code_copy(c, which, d):
        src, dst = ((cg_in, cg), (cu_in, cu))[which]
        to = lax.rem(t + d, m)
        return pltpu.make_async_remote_copy(
            src_ref=src.at[:, pl.ds(al(to * units + c * cw, 128), cw)],
            dst_ref=dst.at[mine, pl.ds(al(c * cw, 128), cw)],
            send_sem=s_code.at[c, which, d], recv_sem=r_code.at[c, which, d],
            device_id={"tp": to}, device_id_type=MESH)

    def down_copy(d):
        to = lax.rem(t + d, m)
        return pltpu.make_async_remote_copy(
            src_ref=cd_in.at[pl.ds(al(to * units, 16), units), :],
            dst_ref=cd.at[:, pl.ds(al(t * dcw, 128), dcw)],
            send_sem=s_down.at[d], recv_sem=r_down.at[d],
            device_id={"tp": to}, device_id_type=MESH)

    def codes_start(first, stop):
        @pl.loop(first, stop)
        def _(c):
            for d in range(1, m):
                code_copy(c, 0, d).start()
                code_copy(c, 1, d).start()

    def normalise(b):
        for d in range(1, m):
            rows_out(b, d).wait_recv()
        values = wide[b].astype(F32)
        inverse = lax.rsqrt(jnp.mean(values * values, axis=1, keepdims=True) + EPSILON)
        normed = (values * inverse * gain_ref[...]).astype(BF16)
        for j in range(n):
            cut[b, j] = normed[:, j * depth:(j + 1) * depth]
        grp[b, pl.ds(al(f * ns, 16), ns), :] = cut[b, f]
        for d in range(1, n):
            normed_out(b, d).start()

    def gather(b):
        for d in range(1, n):
            normed_out(b, d).wait_recv()
        place = lax.broadcasted_iota(jnp.int32, (rp, n * ns), 0) == row_ref[b]
        place = jnp.where(place, 1.0, 0.0).astype(BF16)
        x_ref[my_part(b), :] = jnp.dot(place, grp[b], preferred_element_type=F32).astype(BF16)
        for d in range(1, m):
            x_out(b, d).start()

    pl.semaphore_wait(barrier, m + n - 2)
    for b in range(BLOCKS):
        for d in range(1, m):
            rows_out(b, d).start()
    if here:
        for d in range(1, m):
            scale_copy(d).start()
    early = min(2, chunks)
    codes_start(0, early)
    for b in range(BLOCKS):
        wide[b, :, my_feat] = sent[t, b]
    for b in range(BLOCKS):
        normalise(b)
    gather(0)
    codes_start(early, chunks)
    local[5].wait()
    if here:
        for d in range(1, m):
            scale_copy(d).wait_recv()
    for j in range(depth // 128):
        st[j * 128:(j + 1) * 128, :] = sct[:, j * 128:(j + 1) * 128].T
    for b in range(1, BLOCKS):
        gather(b)
    if here:
        for d in range(1, m):
            scale_down_copy(d).start()
            down_copy(d).start()
    local[0].wait()
    local[1].wait()

    def unpack(c):
        slot = lax.rem(c, 2)

        @pl.when(c + 1 < chunks)
        def _():
            base_start(c + 1, 1 - slot)
        base_copy(c, slot, 0, bg_in).wait()
        base_copy(c, slot, 1, bu_in).wait()
        for d in range(1, m):
            code_copy(c, 0, d).wait_recv()
            code_copy(c, 1, d).wait_recv()
        there = pl.ds(al(c * cw, 128), cw)
        scales = st[...]
        lane = lax.broadcasted_iota(jnp.int32, scales.shape, 1)
        for which, codes in ((0, cg), (1, cu)):
            picked = jnp.where(lane == c + which * chunks, scales, 0.0)
            column = jnp.sum(picked, axis=1, keepdims=True)
            codes[:, there] = (base[slot, which].astype(F32) + codes[:, there].astype(F32) * column).astype(BF16)

    def partial(k):
        b, c = k // chunks, lax.rem(k, chunks)

        @pl.when(c == 0)
        def _():
            for d in range(1, m):
                x_out(b, d).wait_recv()

        @pl.when(b == 0)
        def _():
            unpack(c)
        there = pl.ds(al(c * cw, 128), cw)
        both = jnp.concatenate([cg[:, there], cu[:, there]], axis=1)
        for side in range(2):
            xs = x_ref[pl.ds(al(b * rows + side * half, 16), half), :]
            own[side, k] = jnp.dot(xs, both, preferred_element_type=F32).astype(BF16)

    def spot(k, side):
        b, c = k // chunks, lax.rem(k, chunks)
        return hid.at[pl.ds(al(b * rows + side * half, 16), half), pl.ds(al(c * cw, 128), cw)]

    def red_copy(k, side):
        return pltpu.make_async_remote_copy(
            src_ref=own.at[side, k], dst_ref=got.at[side, k], send_sem=s_red.at[side, k], recv_sem=r_red.at[side, k],
            device_id={"fsdp": jnp.clip(f + (1 if side else -1), 0, last)}, device_id_type=MESH)

    def hid_copy(k, side):
        return pltpu.make_async_remote_copy(
            src_ref=spot(k, side), dst_ref=spot(k, side), send_sem=s_hid.at[side, k], recv_sem=r_hid.at[side, k],
            device_id={"fsdp": jnp.clip(f + (-1 if side else 1), 0, last)}, device_id_type=MESH)

    def valid(k):
        return (k >= 0) & (k < total)

    def reduce_step(s, side):
        far = f if side else last - f
        k = s - far

        @pl.when(valid(k) & (far > 0))
        def _():
            red_copy(k, side).wait_recv()

            @pl.when(far < last)
            def _():
                own[side, k] = (own[side, k].astype(F32) + got[side, k].astype(F32)).astype(BF16)

            @pl.when(far == last)
            def _():
                both = own[side, k].astype(F32) + got[side, k].astype(F32)
                gate, up = both[:, :cw], both[:, cw:]
                b, c = k // chunks, lax.rem(k, chunks)
                hid[pl.ds(al(b * rows + side * half, 16), half), pl.ds(al(c * cw, 128), cw)] = (
                    jax.nn.silu(gate) * up).astype(BF16)

    def reduce_send(s, side):
        far = f if side else last - f
        k = s - far

        @pl.when(valid(k) & (far < last))
        def _():
            red_copy(k, side).start()

        @pl.when(valid(k) & (far == last))
        def _():
            hid_copy(k, side).start()

    def pass_on(s, side):
        far = f if side else last - f
        k = s - last - (last - far)

        @pl.when(valid(k) & (far < last))
        def _():
            hid_copy(k, side).wait_recv()

            @pl.when(far > 0)
            def _():
                hid_copy(k, side).start()

    def down_weights():
        for i in range(2, 5):
            local[i].wait()
        if here:
            for d in range(1, m):
                scale_down_copy(d).wait_recv()
                down_copy(d).wait_recv()

        @pl.loop(0, chunks)
        def _(c):
            there = pl.ds(al(c * cw, 16), cw)
            cd[there, :] = (bd[there, :].astype(F32) + cd[there, :].astype(F32) * sd[pl.ds(c, 1), :]).astype(BF16)

    def down(b):
        for j in reversed(range(m // 2)):
            first = lax.rem(t // 2 + j, m // 2) * 2
            both = jnp.dot(hid[pl.ds(al(b * rows + first * rp, 16), 2 * rp), :], cd[...], preferred_element_type=F32)
            both = both.astype(BF16)
            part_out[b, first] = both[:rp]
            part_out[b, first + 1] = both[rp:]
            for e in range(2):
                d = lax.rem(first + e - t + m, m)
                if j:
                    sum_out(b, d).start()
                else:
                    @pl.when(d > 0)
                    def _():
                        sum_out(b, d).start()

    def send_back(b):
        acc = part_out[b, t].astype(F32)
        for d in range(1, m):
            sum_out(b, d).wait_recv()
        for d in range(1, m):
            acc = acc + part_in[b, lax.rem(t + d, m)].astype(F32)
        place = lax.broadcasted_iota(jnp.int32, (n * ns, rp), 1) == col_ref[b]
        place = jnp.where(place, 1.0, 0.0).astype(BF16)
        spread = jnp.dot(place, acc.astype(BF16), preferred_element_type=F32).astype(BF16)
        for g in range(n):
            back[b, g] = spread[g * ns:(g + 1) * ns]
        for d in range(1, n):
            back_out(b, d).start()
        back_wide[b, :, my_depth] = back[b, f]

    def send_home(b):
        for d in range(1, n):
            back_out(b, d).wait_recv()
        for d in range(1, m):
            home_out(b, d).start()
        out_ref[t, b] = back_wide[b, :, my_feat]

    steps = total + 2 * last
    tasks = [(chunks - 1 + 2 * last, down_weights)]
    for b in range(BLOCKS):
        at = (b + 1) * chunks - 1 + 2 * last
        tasks += [(at, functools.partial(down, b)), (at + 4, functools.partial(send_back, b)),
                  (at + 6, functools.partial(send_home, b))]

    partial(0)

    @pl.loop(0, steps)
    def _(s):
        for side in range(2):
            reduce_step(s, side)
        for side in range(2):
            reduce_send(s, side)
        for side in range(2):
            pass_on(s, side)

        @pl.when(s + 1 < total)
        def _():
            partial(s + 1)
        for at, task in tasks:
            if at < steps:
                pl.when(s == at)(task)

    for at, task in tasks:
        if at >= steps:
            task()
    for b in range(BLOCKS):
        for d in range(1, m):
            home_out(b, d).wait_recv()

    @pl.loop(0, chunks)
    def _(c):
        for d in range(1, m):
            code_copy(c, 0, d).wait_send()
            code_copy(c, 1, d).wait_send()
    if here:
        for d in range(1, m):
            down_copy(d).wait_send()
            scale_copy(d).wait_send()
            scale_down_copy(d).wait_send()
    for b in range(BLOCKS):
        for d in range(1, m):
            for out in (rows_out, x_out, sum_out, home_out):
                out(b, d).wait_send()
        for d in range(1, n):
            for out in (normed_out, back_out):
                out(b, d).wait_send()

    @pl.loop(0, total)
    def _(k):
        for side in range(2):
            far = f if side else last - f

            @pl.when(far < last)
            def _():
                red_copy(k, side).wait_send()

            @pl.when(far > 0)
            def _():
                hid_copy(k, side).wait_send()


def layer(n, m, here, sent, gain, row_of, col_of, code_gate, code_up, scales, base_gate, base_up,
          code_down, scale_down, base_down, live_all):
    width, units = base_gate.shape
    depth = width // n
    ns, feat = sent.shape[2:]
    chunks = scale_down.shape[-2]
    cw = units // chunks
    total = BLOCKS * chunks
    half = live_all // (2 * BLOCKS)
    rp = live_all // (BLOCKS * m)
    anywhere = pl.BlockSpec(memory_space=pl.ANY)
    near = pl.BlockSpec(memory_space=pltpu.VMEM)
    dma = pltpu.SemaphoreType.DMA
    vm = pltpu.VMEM
    return pl.pallas_call(
        functools.partial(layer_kernel, n, m, here),
        out_shape=jax.ShapeDtypeStruct((m, BLOCKS, ns, feat), BF16),
        in_specs=[near, near, near, near] + [anywhere] * 8,
        out_specs=near,
        scratch_shapes=[
            vm((depth, units), BF16), vm((depth, units), BF16), vm((2, 2, depth, cw), BF16),
            vm((2, total, half, 2 * cw), BF16), vm((2, total, half, 2 * cw), BF16),
            vm((live_all, units), BF16), vm((units, depth), BF16), vm((units, depth), BF16),
            vm((live_all, depth), BF16), vm((BLOCKS, ns, width), BF16), vm((BLOCKS, n, ns, depth), BF16),
            vm((BLOCKS, n * ns, depth), BF16), vm((BLOCKS, m, rp, depth), BF16), vm((BLOCKS, m, rp, depth), BF16),
            vm((BLOCKS, n, ns, depth), BF16), vm((BLOCKS, ns, width), BF16),
            vm((depth, 128), F32), vm((128, depth), F32), vm((chunks, depth), F32),
            dma((chunks, 2, m)), dma((chunks, 2, m)), dma((m,)), dma((m,)), dma((6,)), dma((2, 2)),
            dma((2, total)), dma((2, total)), dma((2, total)), dma((2, total)),
            dma((4, BLOCKS, m)), dma((4, BLOCKS, m)), dma((2, BLOCKS, n)), dma((2, BLOCKS, n)), dma((2, m)), dma((2, m)),
        ],
        compiler_params=pltpu.CompilerParams(
            collective_id=0, has_side_effects=True, vmem_limit_bytes=67043328),
    )(sent, gain, row_of, col_of, code_gate, code_up, scales, base_gate, base_up, code_down, scale_down, base_down)


def shards(tokens, norm_gain, base_gate, base_up, base_down, code_gate, code_up,
           scale_gate, scale_up, code_down, scale_down, cu_seqlens):
    n, m = lax.axis_size("fsdp"), lax.axis_size("tp")
    me_f, me_t = lax.axis_index("fsdp"), lax.axis_index("tp")
    cap, feat = tokens.shape
    live_all = n * (cap // 2 + SEQS)
    lanes = BLOCKS * m
    rp = live_all // lanes
    ns = -(-(-(-cap // lanes)) // 16) * 16
    kr = code_gate.shape[0]
    nb = scale_gate.shape[1] // m

    bounds_all = lax.all_gather(cu_seqlens, "fsdp", axis=0, tiled=True)
    counts = bounds_all[:, SEQS]
    starts = jnp.cumsum(counts) - counts
    start, live = starts[me_f], counts[me_f]

    q_of = (jnp.arange(m)[:, None] + m * jnp.arange(BLOCKS)[None, :])
    row_of = ((q_of - start) % lanes)[:, :, None] + lanes * jnp.arange(ns)[None, None, :]
    row_of = jnp.where(row_of < live, row_of, -1).reshape(-1)
    slots = jnp.arange(cap, dtype=jnp.int32)
    spread = (row_of[:, None] == slots[None, :]).astype(BF16)
    sent = jnp.dot(spread, tokens, preferred_element_type=F32).astype(BF16)

    q_mine = me_t + m * jnp.arange(BLOCKS)
    r_all = ((q_mine[:, None] - starts[None, :]) % lanes)[:, :, None] + lanes * jnp.arange(ns)[None, None, :]
    slot_all = jnp.where(r_all < counts[None, :, None], (starts[None, :, None] + r_all) // lanes, -1)
    slot_all = slot_all.reshape(BLOCKS, n * ns)

    scales = jnp.concatenate([scale_gate.reshape(kr, m, nb), scale_up.reshape(kr, m, nb)], axis=2).transpose(1, 2, 0)
    scales = jnp.pad(scales, ((0, 0), (0, -(2 * nb) % 8), (0, 0)))
    scale_down = scale_down.reshape(m, nb, -1)
    here = code_down.shape[1] % 128 == 0 and kr % 128 == 0
    if not here:
        code_down = lax.all_to_all(code_down, "tp", split_axis=0, concat_axis=1, tiled=True)
        scales = lax.all_to_all(scales, "tp", split_axis=0, concat_axis=2, tiled=True)[0]
        scale_down = lax.all_to_all(scale_down, "tp", split_axis=0, concat_axis=2, tiled=True)[0]
    home = layer(n, m, here, sent.reshape(m, BLOCKS, ns, feat), norm_gain[None, :], slot_all[:, None, :],
                 slot_all[:, :, None], code_gate, code_up, scales, base_gate, base_up, code_down, scale_down,
                 base_down, live_all)
    summed_out = lax.dot_general(spread, home.reshape(m * BLOCKS * ns, feat), (((0,), (0,)), ((), ())),
                                 preferred_element_type=F32)

    bounds = cu_seqlens[0]
    mixed = (tokens.astype(F32) + summed_out).astype(BF16)
    mixed = jnp.where((slots < live)[:, None], mixed, jnp.zeros((), BF16))
    member = (slots[None, :] >= bounds[:-1, None]) & (slots[None, :] < bounds[1:, None])
    seq_sums = jnp.dot(member.astype(BF16), mixed, preferred_element_type=F32)
    lengths = (bounds[1:] - bounds[:-1]).astype(F32)
    return mixed, seq_sums / lengths[:, None]


def solution(mesh):
    placed = (
        P("fsdp", "tp"), P(), P(None, "tp"), P(None, "tp"), P("tp", None),
        P(("fsdp", "tp"), None), P(("fsdp", "tp"), None),
        P(("fsdp", "tp"), None), P(("fsdp", "tp"), None),
        P(None, ("fsdp", "tp")), P(None, ("fsdp", "tp")), P("fsdp", None),
    )
    return jax.shard_map(shards, mesh=mesh, in_specs=placed,
                         out_specs=(P("fsdp", "tp"), P("fsdp", "tp")), check_vma=False)
```

```python
import functools
import jax
import jax.numpy as jnp
from jax import lax
from jax.experimental import pallas as pl
from jax.experimental.pallas import tpu as pltpu
from jax.sharding import PartitionSpec as P

SEQS = 8
EPSILON = 1e-06
BLOCKS = 2
SUB = 2
F32, BF16 = jnp.float32, jnp.bfloat16
MESH = pl.DeviceIdType.MESH


def al(value, size):
    return pl.multiple_of(value, size)


def layer_kernel(n, m, here, *refs):
    (sent, gain_ref, row_ref, col_ref, cg_in, cu_in, sg_in, bg_in, bu_in, cd_in, sd_in, bd_in, out_ref,
     cg, cu, base, own, got, hid, cd, bd, x_ref, wide, cut, grp, part_out, part_in, back, back_wide, st, sct, sd,
     s_code, r_code, s_down, r_down, l_sem, b_sem, s_red, r_red, s_hid, r_hid, s_x, r_x,
     s_tp, r_tp, s_fs, r_fs, s_sc, r_sc) = refs
    f, t = lax.axis_index("fsdp"), lax.axis_index("tp")
    kr = cg_in.shape[0]
    depth, units = cg.shape
    cw = base.shape[3]
    chunks = units // cw
    rows = x_ref.shape[0] // BLOCKS
    half = rows // 2
    rp = rows // m
    ns, feat = sent.shape[2], sent.shape[3]
    nb2 = sg_in.shape[-2]
    total = BLOCKS * chunks
    last = n - 1
    dcw = depth // m

    barrier = pltpu.get_barrier_semaphore()
    for d in range(1, m):
        pl.semaphore_signal(barrier, inc=1, device_id={"tp": lax.rem(t + d, m)}, device_id_type=MESH)
    for d in range(1, n):
        pl.semaphore_signal(barrier, inc=1, device_id={"fsdp": lax.rem(f + d, n)}, device_id_type=MESH)

    def base_copy(c, slot, which, src):
        return pltpu.make_async_copy(
            src.at[pl.ds(al(f * depth, 16), depth), pl.ds(al(c * cw, 128), cw)],
            base.at[slot, which], b_sem.at[slot, which])

    def base_start(c, slot):
        base_copy(c, slot, 0, bg_in).start()
        base_copy(c, slot, 1, bu_in).start()

    mine = pl.ds(al(t * kr, 16), kr)
    cols = pl.ds(al(t * units, 128), units)
    local = [pltpu.make_async_copy(cg_in.at[:, cols], cg.at[mine, :], l_sem.at[0]),
             pltpu.make_async_copy(cu_in.at[:, cols], cu.at[mine, :], l_sem.at[1]),
             pltpu.make_async_copy(bd_in.at[:, pl.ds(al(f * depth, 128), depth)], bd, l_sem.at[2])]
    if here:
        local += [pltpu.make_async_copy(
            cd_in.at[pl.ds(al(t * units, 16), units), :], cd.at[:, pl.ds(al(t * dcw, 128), dcw)], l_sem.at[3]),
            pltpu.make_async_copy(sd_in.at[t], sd.at[:, pl.ds(al(t * dcw, 128), dcw)], l_sem.at[4]),
            pltpu.make_async_copy(sg_in.at[t], sct.at[0:nb2, pl.ds(al(t * kr, 128), kr)], l_sem.at[5])]
    else:
        local += [pltpu.make_async_copy(cd_in, cd, l_sem.at[3]), pltpu.make_async_copy(sd_in, sd, l_sem.at[4]),
                  pltpu.make_async_copy(sg_in, sct.at[0:nb2, :], l_sem.at[5])]
    base_start(0, 0)
    if nb2 < sct.shape[0]:
        sct[nb2:, :] = jnp.zeros_like(sct[nb2:, :])
    for copy in local:
        copy.start()

    def to_tp(b, stage, d, src, dst):
        return pltpu.make_async_remote_copy(
            src_ref=src, dst_ref=dst, send_sem=s_tp.at[stage, b, d], recv_sem=r_tp.at[stage, b, d],
            device_id={"tp": lax.rem(t + d, m)}, device_id_type=MESH)

    def to_fs(b, stage, d, src, dst):
        return pltpu.make_async_remote_copy(
            src_ref=src, dst_ref=dst, send_sem=s_fs.at[stage, b, d], recv_sem=r_fs.at[stage, b, d],
            device_id={"fsdp": lax.rem(f + d, n)}, device_id_type=MESH)

    my_feat = pl.ds(al(t * feat, 128), feat)
    my_depth = pl.ds(al(f * depth, 128), depth)

    def my_part(b):
        return pl.ds(al(b * rows + t * rp, 16), rp)

    def rows_out(b, d):
        return to_tp(b, 0, d, sent.at[lax.rem(t + d, m), b], wide.at[b, :, my_feat])

    def normed_out(b, d):
        return to_fs(b, 0, d, cut.at[b, lax.rem(f + d, n)], grp.at[b, pl.ds(al(f * ns, 16), ns), :])

    def flip(bits):
        peer, bit = t, 1
        while bit <= bits:
            if bits & bit:
                peer = peer + bit - 2 * bit * lax.rem(t // bit, 2)
            bit *= 2
        return peer

    def x_copy(b, h, mask, bit):
        spot = x_ref.at[pl.ds(al(b * rows + flip(mask) * rp + h * (rp // 2), 16), rp // 2), :]
        return pltpu.make_async_remote_copy(
            src_ref=spot, dst_ref=spot, send_sem=s_x.at[b, h, mask ^ bit], recv_sem=r_x.at[b, h, mask ^ bit],
            device_id={"tp": flip(bit)}, device_id_type=MESH)

    def x_arrived(b, h, mask):
        spot = x_ref.at[pl.ds(al(b * rows + flip(mask) * rp + h * (rp // 2), 16), rp // 2), :]
        pltpu.make_async_remote_copy(
            src_ref=spot, dst_ref=spot, send_sem=s_x.at[b, h, mask], recv_sem=r_x.at[b, h, mask],
            device_id={"tp": flip(1)}, device_id_type=MESH).wait_recv()

    far_bits = [2 ** i for i in range(1, m.bit_length() - 1)]
    far_masks = sorted(range(2, m, 2), key=lambda mask: (bin(mask).count("1"), mask))
    orders = (far_bits, far_bits[::-1])

    def onward(h, mask):
        order = orders[h]
        used = [i for i, bit in enumerate(order) if mask & bit]
        return order[max(used, default=-1) + 1:]

    def relay(b, phase):
        for mask in [0] + far_masks:
            if bin(mask).count("1") == phase:
                for h in range(2):
                    if mask:
                        x_arrived(b, h, mask)
                    for bit in onward(h, mask) + [1]:
                        x_copy(b, h, mask, bit).start()

    def x_wait(b):
        for mask in range(1, m, 2):
            for h in range(2):
                x_arrived(b, h, mask)

    def x_sent(b):
        for mask in [0] + far_masks:
            for h in range(2):
                for bit in onward(h, mask) + [1]:
                    x_copy(b, h, mask, bit).wait_send()

    def sum_out(b, d):
        return to_tp(b, 2, d, part_out.at[b, lax.rem(t + d, m)], part_in.at[b, t])

    def back_out(b, d):
        return to_fs(b, 1, d, back.at[b, lax.rem(f + d, n)], back_wide.at[b, :, my_depth])

    def home_out(b, d):
        return to_tp(b, 3, d, back_wide.at[b, :, pl.ds(al(lax.rem(t + d, m) * feat, 128), feat)], out_ref.at[t, b])

    def scale_copy(d):
        to = lax.rem(t + d, m)
        return pltpu.make_async_remote_copy(
            src_ref=sg_in.at[to], dst_ref=sct.at[0:nb2, pl.ds(al(t * kr, 128), kr)],
            send_sem=s_sc.at[0, d], recv_sem=r_sc.at[0, d], device_id={"tp": to}, device_id_type=MESH)

    def scale_down_copy(d):
        to = lax.rem(t + d, m)
        return pltpu.make_async_remote_copy(
            src_ref=sd_in.at[to], dst_ref=sd.at[:, pl.ds(al(t * dcw, 128), dcw)],
            send_sem=s_sc.at[1, d], recv_sem=r_sc.at[1, d], device_id={"tp": to}, device_id_type=MESH)

    def code_copy(c, which, d):
        src, dst = ((cg_in, cg), (cu_in, cu))[which]
        to = lax.rem(t + d, m)
        return pltpu.make_async_remote_copy(
            src_ref=src.at[:, pl.ds(al(to * units + c * cw, 128), cw)],
            dst_ref=dst.at[mine, pl.ds(al(c * cw, 128), cw)],
            send_sem=s_code.at[c, which, d], recv_sem=r_code.at[c, which, d],
            device_id={"tp": to}, device_id_type=MESH)

    def down_copy(d):
        to = lax.rem(t + d, m)
        return pltpu.make_async_remote_copy(
            src_ref=cd_in.at[pl.ds(al(to * units, 16), units), :],
            dst_ref=cd.at[:, pl.ds(al(t * dcw, 128), dcw)],
            send_sem=s_down.at[d], recv_sem=r_down.at[d],
            device_id={"tp": to}, device_id_type=MESH)

    def codes_start(c):
        for d in range(1, m):
            code_copy(c, 0, d).start()
            code_copy(c, 1, d).start()

    def normalise(b):
        for d in range(1, m):
            rows_out(b, d).wait_recv()
        values = wide[b].astype(F32)
        inverse = lax.rsqrt(jnp.mean(values * values, axis=1, keepdims=True) + EPSILON)
        normed = (values * inverse * gain_ref[...]).astype(BF16)
        for j in range(n):
            cut[b, j] = normed[:, j * depth:(j + 1) * depth]
        grp[b, pl.ds(al(f * ns, 16), ns), :] = cut[b, f]
        for d in range(1, n):
            normed_out(b, d).start()

    def gather(b):
        for d in range(1, n):
            normed_out(b, d).wait_recv()
        place = lax.broadcasted_iota(jnp.int32, (rp, n * ns), 0) == row_ref[b]
        place = jnp.where(place, 1.0, 0.0).astype(BF16)
        x_ref[my_part(b), :] = jnp.dot(place, grp[b], preferred_element_type=F32).astype(BF16)
        relay(b, 0)

    pl.semaphore_wait(barrier, m + n - 2)
    for b in range(BLOCKS):
        for d in range(1, m):
            rows_out(b, d).start()
    if here:
        for d in range(1, m):
            scale_copy(d).start()
            scale_down_copy(d).start()
    codes_start(0)
    for b in range(BLOCKS):
        wide[b, :, my_feat] = sent[t, b]
    for b in range(BLOCKS):
        normalise(b)
    gather(0)
    local[5].wait()
    if here:
        for d in range(1, m):
            scale_copy(d).wait_recv()
    for j in range(depth // 128):
        st[j * 128:(j + 1) * 128, :] = sct[:, j * 128:(j + 1) * 128].T
    for phase in range(1, len(far_bits) + 1):
        relay(0, phase)
    ahead = min(3, chunks)
    for c in range(1, ahead):
        codes_start(c)
    local[0].wait()
    local[1].wait()

    def unpack(c):
        slot = lax.rem(c, 2)

        @pl.when(c + 1 < chunks)
        def _():
            base_start(c + 1, 1 - slot)
        base_copy(c, slot, 0, bg_in).wait()
        base_copy(c, slot, 1, bu_in).wait()
        for d in range(1, m):
            code_copy(c, 0, d).wait_recv()
            code_copy(c, 1, d).wait_recv()
        there = pl.ds(al(c * cw, 128), cw)
        scales = st[...]
        lane = lax.broadcasted_iota(jnp.int32, scales.shape, 1)
        for which, codes in ((0, cg), (1, cu)):
            picked = jnp.where(lane == c + which * chunks, scales, 0.0)
            column = jnp.sum(picked, axis=1, keepdims=True)
            codes[:, there] = (base[slot, which].astype(F32) + codes[:, there].astype(F32) * column).astype(BF16)

    def partial(k):
        b, c = k // chunks, lax.rem(k, chunks)

        @pl.when(c == 0)
        def _():
            x_wait(b)

        @pl.when(b == 0)
        def _():
            unpack(c)
        there = pl.ds(al(c * cw, 128), cw)
        both = jnp.concatenate([cg[:, there], cu[:, there]], axis=1)
        for side in range(2):
            xs = x_ref[pl.ds(al(b * rows + side * half, 16), half), :]
            own[side, k] = jnp.dot(xs, both, preferred_element_type=F32).astype(BF16)

    piece = half // SUB

    def spot(k, side, u):
        b, c = k // chunks, lax.rem(k, chunks)
        return hid.at[pl.ds(al(b * rows + side * half + u * piece, 16), piece), pl.ds(al(c * cw, 128), cw)]

    def red_copy(k, side, u):
        there = pl.ds(u * piece, piece)
        return pltpu.make_async_remote_copy(
            src_ref=own.at[side, k, there, :], dst_ref=got.at[side, k, there, :],
            send_sem=s_red.at[side, k, u], recv_sem=r_red.at[side, k, u],
            device_id={"fsdp": jnp.clip(f + (1 if side else -1), 0, last)}, device_id_type=MESH)

    def hid_copy(k, side, u):
        return pltpu.make_async_remote_copy(
            src_ref=spot(k, side, u), dst_ref=spot(k, side, u),
            send_sem=s_hid.at[side, k, u], recv_sem=r_hid.at[side, k, u],
            device_id={"fsdp": jnp.clip(f + (-1 if side else 1), 0, last)}, device_id_type=MESH)

    def valid(k):
        return (k >= 0) & (k < total)

    def reduce_step(s, side, u):
        far = f if side else last - f
        k = s - far
        there = pl.ds(u * piece, piece)

        @pl.when(valid(k) & (far > 0))
        def _():
            red_copy(k, side, u).wait_recv()

            @pl.when(far < last)
            def _():
                own[side, k, there] = (own[side, k, there].astype(F32) + got[side, k, there].astype(F32)).astype(BF16)

            @pl.when(far == last)
            def _():
                both = own[side, k, there].astype(F32) + got[side, k, there].astype(F32)
                gate, up = both[:, :cw], both[:, cw:]
                b, c = k // chunks, lax.rem(k, chunks)
                hid[pl.ds(al(b * rows + side * half + u * piece, 16), piece), pl.ds(al(c * cw, 128), cw)] = (
                    jax.nn.silu(gate) * up).astype(BF16)

    def reduce_send(s, side, u):
        far = f if side else last - f
        k = s - far

        @pl.when(valid(k) & (far < last))
        def _():
            red_copy(k, side, u).start()

        @pl.when(valid(k) & (far == last))
        def _():
            hid_copy(k, side, u).start()

    def pass_on(s, side, u):
        far = f if side else last - f
        k = s - last - (last - far)

        @pl.when(valid(k) & (far < last))
        def _():
            hid_copy(k, side, u).wait_recv()

            @pl.when(far > 0)
            def _():
                hid_copy(k, side, u).start()

    def down_weights():
        for i in range(2, 5):
            local[i].wait()
        if here:
            for d in range(1, m):
                scale_down_copy(d).wait_recv()
                down_copy(d).wait_recv()

        @pl.loop(0, chunks)
        def _(c):
            there = pl.ds(al(c * cw, 16), cw)
            cd[there, :] = (bd[there, :].astype(F32) + cd[there, :].astype(F32) * sd[pl.ds(c, 1), :]).astype(BF16)

    def down(b):
        for j in reversed(range(m // 2)):
            first = lax.rem(t // 2 + j, m // 2) * 2
            both = jnp.dot(hid[pl.ds(al(b * rows + first * rp, 16), 2 * rp), :], cd[...], preferred_element_type=F32)
            both = both.astype(BF16)
            part_out[b, first] = both[:rp]
            part_out[b, first + 1] = both[rp:]
            for e in range(2):
                d = lax.rem(first + e - t + m, m)
                if j:
                    sum_out(b, d).start()
                else:
                    @pl.when(d > 0)
                    def _():
                        sum_out(b, d).start()

    def send_back(b):
        acc = part_out[b, t].astype(F32)
        for d in range(1, m):
            sum_out(b, d).wait_recv()
        for d in range(1, m):
            acc = acc + part_in[b, lax.rem(t + d, m)].astype(F32)
        place = lax.broadcasted_iota(jnp.int32, (n * ns, rp), 1) == col_ref[b]
        place = jnp.where(place, 1.0, 0.0).astype(BF16)
        spread = jnp.dot(place, acc.astype(BF16), preferred_element_type=F32).astype(BF16)
        for g in range(n):
            back[b, g] = spread[g * ns:(g + 1) * ns]
        for d in range(1, n):
            back_out(b, d).start()
        back_wide[b, :, my_depth] = back[b, f]

    def send_home(b):
        for d in range(1, n):
            back_out(b, d).wait_recv()
        for d in range(1, m):
            home_out(b, d).start()
        out_ref[t, b] = back_wide[b, :, my_feat]

    steps = total + 2 * last
    tasks = [(chunks - 1 + 2 * last, down_weights)]
    for b in range(1, BLOCKS):
        tasks.append((1, functools.partial(gather, b)))
        for phase in range(1, len(far_bits) + 1):
            tasks.append((1 + 2 * phase, functools.partial(relay, b, phase)))
    if here:
        for d in range(1, m):
            tasks.append((max(chunks - ahead, 0) + d, down_copy(d).start))
    for b in range(BLOCKS):
        at = (b + 1) * chunks - 1 + 2 * last
        tasks += [(at, functools.partial(down, b)), (at + 4, functools.partial(send_back, b)),
                  (at + 6, functools.partial(send_home, b))]

    partial(0)

    @pl.loop(0, steps)
    def _(s):
        for u in range(SUB):
            for side in range(2):
                reduce_step(s, side, u)
            for side in range(2):
                reduce_send(s, side, u)
        for u in range(SUB):
            for side in range(2):
                pass_on(s, side, u)

        @pl.when(s + ahead < chunks)
        def _():
            codes_start(s + ahead)

        @pl.when(s + 1 < total)
        def _():
            partial(s + 1)
        for at, task in tasks:
            if at < steps:
                pl.when(s == at)(task)

    for at, task in tasks:
        if at >= steps:
            task()
    for b in range(BLOCKS):
        for d in range(1, m):
            home_out(b, d).wait_recv()

    @pl.loop(0, chunks)
    def _(c):
        for d in range(1, m):
            code_copy(c, 0, d).wait_send()
            code_copy(c, 1, d).wait_send()
    if here:
        for d in range(1, m):
            down_copy(d).wait_send()
            scale_copy(d).wait_send()
            scale_down_copy(d).wait_send()
    for b in range(BLOCKS):
        for d in range(1, m):
            for out in (rows_out, sum_out, home_out):
                out(b, d).wait_send()
        x_sent(b)
        for d in range(1, n):
            for out in (normed_out, back_out):
                out(b, d).wait_send()

    @pl.loop(0, total)
    def _(k):
        for side in range(2):
            far = f if side else last - f

            @pl.when(far < last)
            def _():
                for u in range(SUB):
                    red_copy(k, side, u).wait_send()

            @pl.when(far > 0)
            def _():
                for u in range(SUB):
                    hid_copy(k, side, u).wait_send()


def layer(n, m, here, sent, gain, row_of, col_of, code_gate, code_up, scales, base_gate, base_up,
          code_down, scale_down, base_down, live_all):
    width, units = base_gate.shape
    depth = width // n
    ns, feat = sent.shape[2:]
    chunks = scale_down.shape[-2]
    cw = units // chunks
    total = BLOCKS * chunks
    half = live_all // (2 * BLOCKS)
    rp = live_all // (BLOCKS * m)
    anywhere = pl.BlockSpec(memory_space=pl.ANY)
    near = pl.BlockSpec(memory_space=pltpu.VMEM)
    dma = pltpu.SemaphoreType.DMA
    vm = pltpu.VMEM
    return pl.pallas_call(
        functools.partial(layer_kernel, n, m, here),
        out_shape=jax.ShapeDtypeStruct((m, BLOCKS, ns, feat), BF16),
        in_specs=[near, near, near, near] + [anywhere] * 8,
        out_specs=near,
        scratch_shapes=[
            vm((depth, units), BF16), vm((depth, units), BF16), vm((2, 2, depth, cw), BF16),
            vm((2, total, half, 2 * cw), BF16), vm((2, total, half, 2 * cw), BF16),
            vm((live_all, units), BF16), vm((units, depth), BF16), vm((units, depth), BF16),
            vm((live_all, depth), BF16), vm((BLOCKS, ns, width), BF16), vm((BLOCKS, n, ns, depth), BF16),
            vm((BLOCKS, n * ns, depth), BF16), vm((BLOCKS, m, rp, depth), BF16), vm((BLOCKS, m, rp, depth), BF16),
            vm((BLOCKS, n, ns, depth), BF16), vm((BLOCKS, ns, width), BF16),
            vm((depth, 128), F32), vm((128, depth), F32), vm((chunks, depth), F32),
            dma((chunks, 2, m)), dma((chunks, 2, m)), dma((m,)), dma((m,)), dma((6,)), dma((2, 2)),
            dma((2, total, SUB)), dma((2, total, SUB)), dma((2, total, SUB)), dma((2, total, SUB)),
            dma((BLOCKS, 2, m)), dma((BLOCKS, 2, m)),
            dma((4, BLOCKS, m)), dma((4, BLOCKS, m)), dma((2, BLOCKS, n)), dma((2, BLOCKS, n)), dma((2, m)), dma((2, m)),
        ],
        compiler_params=pltpu.CompilerParams(
            collective_id=0, has_side_effects=True, vmem_limit_bytes=67043328),
    )(sent, gain, row_of, col_of, code_gate, code_up, scales, base_gate, base_up, code_down, scale_down, base_down)


def shards(tokens, norm_gain, base_gate, base_up, base_down, code_gate, code_up,
           scale_gate, scale_up, code_down, scale_down, cu_seqlens):
    n, m = lax.axis_size("fsdp"), lax.axis_size("tp")
    me_f, me_t = lax.axis_index("fsdp"), lax.axis_index("tp")
    cap, feat = tokens.shape
    live_all = n * (cap // 2 + SEQS)
    lanes = BLOCKS * m
    rp = live_all // lanes
    ns = -(-(-(-cap // lanes)) // 16) * 16
    kr = code_gate.shape[0]
    nb = scale_gate.shape[1] // m

    bounds_all = lax.all_gather(cu_seqlens, "fsdp", axis=0, tiled=True)
    counts = bounds_all[:, SEQS]
    starts = jnp.cumsum(counts) - counts
    start, live = starts[me_f], counts[me_f]

    q_of = (jnp.arange(m)[:, None] + m * jnp.arange(BLOCKS)[None, :])
    row_of = ((q_of - start) % lanes)[:, :, None] + lanes * jnp.arange(ns)[None, None, :]
    row_of = jnp.where(row_of < live, row_of, -1).reshape(-1)
    slots = jnp.arange(cap, dtype=jnp.int32)
    spread = (row_of[:, None] == slots[None, :]).astype(BF16)
    sent = jnp.dot(spread, tokens, preferred_element_type=F32).astype(BF16)

    q_mine = me_t + m * jnp.arange(BLOCKS)
    r_all = ((q_mine[:, None] - starts[None, :]) % lanes)[:, :, None] + lanes * jnp.arange(ns)[None, None, :]
    slot_all = jnp.where(r_all < counts[None, :, None], (starts[None, :, None] + r_all) // lanes, -1)
    slot_all = slot_all.reshape(BLOCKS, n * ns)

    scales = jnp.concatenate([scale_gate.reshape(kr, m, nb), scale_up.reshape(kr, m, nb)], axis=2).transpose(1, 2, 0)
    scales = jnp.pad(scales, ((0, 0), (0, -(2 * nb) % 8), (0, 0)))
    scale_down = scale_down.reshape(m, nb, -1)
    here = code_down.shape[1] % 128 == 0 and kr % 128 == 0
    if not here:
        code_down = lax.all_to_all(code_down, "tp", split_axis=0, concat_axis=1, tiled=True)
        scales = lax.all_to_all(scales, "tp", split_axis=0, concat_axis=2, tiled=True)[0]
        scale_down = lax.all_to_all(scale_down, "tp", split_axis=0, concat_axis=2, tiled=True)[0]
    home = layer(n, m, here, sent.reshape(m, BLOCKS, ns, feat), norm_gain[None, :], slot_all[:, None, :],
                 slot_all[:, :, None], code_gate, code_up, scales, base_gate, base_up, code_down, scale_down,
                 base_down, live_all)
    summed_out = lax.dot_general(spread, home.reshape(m * BLOCKS * ns, feat), (((0,), (0,)), ((), ())),
                                 preferred_element_type=F32)

    bounds = cu_seqlens[0]
    mixed = (tokens.astype(F32) + summed_out).astype(BF16)
    mixed = jnp.where((slots < live)[:, None], mixed, jnp.zeros((), BF16))
    member = (slots[None, :] >= bounds[:-1, None]) & (slots[None, :] < bounds[1:, None])
    seq_sums = jnp.dot(member.astype(BF16), mixed, preferred_element_type=F32)
    lengths = (bounds[1:] - bounds[:-1]).astype(F32)
    return mixed, seq_sums / lengths[:, None]


def solution(mesh):
    placed = (
        P("fsdp", "tp"), P(), P(None, "tp"), P(None, "tp"), P("tp", None),
        P(("fsdp", "tp"), None), P(("fsdp", "tp"), None),
        P(("fsdp", "tp"), None), P(("fsdp", "tp"), None),
        P(None, ("fsdp", "tp")), P(None, ("fsdp", "tp")), P("fsdp", None),
    )
    return jax.shard_map(shards, mesh=mesh, in_specs=placed,
                         out_specs=(P("fsdp", "tp"), P("fsdp", "tp")), check_vma=False)
```

```python
import functools
import jax
import jax.numpy as jnp
from jax import lax
from jax.experimental import pallas as pl
from jax.experimental.pallas import tpu as pltpu
from jax.sharding import PartitionSpec as P

SEQS = 8
EPSILON = 1e-06
BLOCKS = 2
SUB = 2
QUARTERS = 4
F32, BF16 = jnp.float32, jnp.bfloat16
MESH = pl.DeviceIdType.MESH


def al(value, size):
    return pl.multiple_of(value, size)


def layer_kernel(n, m, here, *refs):
    (tok_ref, gain_ref, cu_ref, cg_in, cu_in, sg_in, bg_in, bu_in, cd_in, sd_in, bd_in, out_ref,
     cg, cu, base, own, got, hid, cd, bd, x_ref, wide, cut, grp, part_out, part_in, back, back_wide, st, sct, sd,
     sent, home, bounds,
     s_code, r_code, s_down, r_down, l_sem, b_sem, s_red, r_red, s_hid, r_hid, s_x, r_x,
     s_tp, r_tp, s_fs, r_fs, s_sc, r_sc, s_sum, r_sum, s_back, r_back, s_bound, r_bound) = refs
    f, t = lax.axis_index("fsdp"), lax.axis_index("tp")
    kr = cg_in.shape[0]
    depth, units = cg.shape
    cw = base.shape[3]
    chunks = units // cw
    rows = x_ref.shape[0] // BLOCKS
    half = rows // 2
    rp = rows // m
    cap, feat = tok_ref.shape
    ns = wide.shape[1]
    lanes = BLOCKS * m
    lane_bits, part_bits = lanes.bit_length() - 1, m.bit_length() - 1
    dq = depth // QUARTERS
    per = QUARTERS // (m // n)
    nb2 = sg_in.shape[-2]
    total = BLOCKS * chunks
    last = n - 1
    dcw = depth // m

    barrier = pltpu.get_barrier_semaphore()
    for d in range(1, m):
        pl.semaphore_signal(barrier, inc=1, device_id={"tp": lax.rem(t + d, m)}, device_id_type=MESH)
    for d in range(1, n):
        pl.semaphore_signal(barrier, inc=1, device_id={"fsdp": lax.rem(f + d, n)}, device_id_type=MESH)

    def base_copy(c, slot, which, src):
        return pltpu.make_async_copy(
            src.at[pl.ds(al(f * depth, 16), depth), pl.ds(al(c * cw, 128), cw)],
            base.at[slot, which], b_sem.at[slot, which])

    def base_start(c, slot):
        base_copy(c, slot, 0, bg_in).start()
        base_copy(c, slot, 1, bu_in).start()

    mine = pl.ds(al(t * kr, 16), kr)
    cols = pl.ds(al(t * units, 128), units)
    local = [pltpu.make_async_copy(cg_in.at[:, cols], cg.at[mine, :], l_sem.at[0]),
             pltpu.make_async_copy(cu_in.at[:, cols], cu.at[mine, :], l_sem.at[1]),
             pltpu.make_async_copy(bd_in.at[:, pl.ds(al(f * depth, 128), depth)], bd, l_sem.at[2])]
    if here:
        local += [pltpu.make_async_copy(
            cd_in.at[pl.ds(al(t * units, 16), units), :], cd.at[:, pl.ds(al(t * dcw, 128), dcw)], l_sem.at[3]),
            pltpu.make_async_copy(sd_in.at[t], sd.at[:, pl.ds(al(t * dcw, 128), dcw)], l_sem.at[4]),
            pltpu.make_async_copy(sg_in.at[t], sct.at[0:nb2, pl.ds(al(t * kr, 128), kr)], l_sem.at[5])]
    else:
        local += [pltpu.make_async_copy(cd_in, cd, l_sem.at[3]), pltpu.make_async_copy(sd_in, sd, l_sem.at[4]),
                  pltpu.make_async_copy(sg_in, sct.at[0:nb2, :], l_sem.at[5])]
    base_start(0, 0)
    if nb2 < sct.shape[0]:
        sct[nb2:, :] = jnp.zeros_like(sct[nb2:, :])
    for copy in local:
        copy.start()

    def to_tp(b, stage, d, src, dst):
        return pltpu.make_async_remote_copy(
            src_ref=src, dst_ref=dst, send_sem=s_tp.at[stage, b, d], recv_sem=r_tp.at[stage, b, d],
            device_id={"tp": lax.rem(t + d, m)}, device_id_type=MESH)

    def to_fs(b, stage, d, src, dst):
        return pltpu.make_async_remote_copy(
            src_ref=src, dst_ref=dst, send_sem=s_fs.at[stage, b, d], recv_sem=r_fs.at[stage, b, d],
            device_id={"fsdp": lax.rem(f + d, n)}, device_id_type=MESH)

    my_feat = pl.ds(al(t * feat, 128), feat)
    my_depth = pl.ds(al(f * depth, 128), depth)

    def my_part(b):
        return pl.ds(al(b * rows + t * rp, 16), rp)

    def home_rows(part, b):
        return pl.ds(al((part * BLOCKS + b) * ns, 16), ns)

    def rows_out(b, d):
        return to_tp(b, 0, d, sent.at[home_rows(lax.rem(t + d, m), b), :], wide.at[b, :, my_feat])

    def normed_out(b, d):
        return to_fs(b, 0, d, cut.at[b, lax.rem(f + d, n)], grp.at[b, pl.ds(al(f * ns, 16), ns), :])

    def flip(bits):
        peer, bit = t, 1
        while bit <= bits:
            if bits & bit:
                peer = peer + bit - 2 * bit * lax.rem(t // bit, 2)
            bit *= 2
        return peer

    def x_copy(b, h, mask, bit):
        spot = x_ref.at[pl.ds(al(b * rows + flip(mask) * rp + h * (rp // 2), 16), rp // 2), :]
        return pltpu.make_async_remote_copy(
            src_ref=spot, dst_ref=spot, send_sem=s_x.at[b, h, mask ^ bit], recv_sem=r_x.at[b, h, mask ^ bit],
            device_id={"tp": flip(bit)}, device_id_type=MESH)

    def x_arrived(b, h, mask):
        spot = x_ref.at[pl.ds(al(b * rows + flip(mask) * rp + h * (rp // 2), 16), rp // 2), :]
        pltpu.make_async_remote_copy(
            src_ref=spot, dst_ref=spot, send_sem=s_x.at[b, h, mask], recv_sem=r_x.at[b, h, mask],
            device_id={"tp": flip(1)}, device_id_type=MESH).wait_recv()

    far_bits = [2 ** i for i in range(1, m.bit_length() - 1)]
    far_masks = sorted(range(2, m, 2), key=lambda mask: (bin(mask).count("1"), mask))
    orders = (far_bits, far_bits[::-1])

    def onward(h, mask):
        order = orders[h]
        used = [i for i, bit in enumerate(order) if mask & bit]
        return order[max(used, default=-1) + 1:]

    def relay(b, phase):
        for mask in [0] + far_masks:
            if bin(mask).count("1") == phase:
                for h in range(2):
                    if mask:
                        x_arrived(b, h, mask)
                    for bit in onward(h, mask) + [1]:
                        x_copy(b, h, mask, bit).start()

    def x_wait(b):
        for mask in range(1, m, 2):
            for h in range(2):
                x_arrived(b, h, mask)

    def x_sent(b):
        for mask in [0] + far_masks:
            for h in range(2):
                for bit in onward(h, mask) + [1]:
                    x_copy(b, h, mask, bit).wait_send()

    def sum_out(b, q, d):
        return pltpu.make_async_remote_copy(
            src_ref=part_out.at[b, q, pl.ds(al(lax.rem(t + d, m) * rp, 16), rp), :], dst_ref=part_in.at[b, q, t],
            send_sem=s_sum.at[b, q, d], recv_sem=r_sum.at[b, q, d],
            device_id={"tp": lax.rem(t + d, m)}, device_id_type=MESH)

    def quarter(q):
        return pl.ds(al(f * depth + q * dq, 128), dq)

    def back_out(b, q, d):
        return pltpu.make_async_remote_copy(
            src_ref=back.at[b, q, lax.rem(f + d, n)], dst_ref=back_wide.at[b, :, quarter(q)],
            send_sem=s_back.at[b, q, d], recv_sem=r_back.at[b, q, d],
            device_id={"fsdp": lax.rem(f + d, n)}, device_id_type=MESH)

    def home_out(b, d):
        return to_tp(b, 1, d, back_wide.at[b, :, pl.ds(al(lax.rem(t + d, m) * feat, 128), feat)],
                     home.at[home_rows(t, b), :])

    def bound_copy(d):
        return pltpu.make_async_remote_copy(
            src_ref=cu_ref, dst_ref=bounds.at[f], send_sem=s_bound.at[d], recv_sem=r_bound.at[d],
            device_id={"fsdp": lax.rem(f + d, n)}, device_id_type=MESH)

    def group_counts():
        counts = [bounds[g][:, SEQS:SEQS + 1] for g in range(n)]
        starts = [jnp.zeros_like(counts[0])]
        for g in range(1, n):
            starts.append(starts[-1] + counts[g - 1])
        return starts, counts

    def home_index(axis):
        starts, counts = group_counts()
        start = sum(jnp.where(f == g, starts[g], 0) for g in range(n))
        live = sum(jnp.where(f == g, counts[g], 0) for g in range(n))
        shape = (cap, 1) if axis == 0 else (1, cap)
        r = lax.broadcasted_iota(jnp.int32, shape, axis)
        lane = (r + start) & (lanes - 1)
        index = ((lane & (m - 1)) * BLOCKS + (lane >> part_bits)) * ns + (r >> lane_bits)
        return jnp.where(r < live, index, -1)

    def slot_index(b, g, axis):
        starts, counts = group_counts()
        shape = (ns, 1) if axis == 0 else (1, ns)
        r = ((t + m * b - starts[g]) & (lanes - 1)) + lanes * lax.broadcasted_iota(jnp.int32, shape, axis)
        return jnp.where(r < counts[g], (starts[g] + r) >> lane_bits, -1)

    def ones_at(mask):
        return jnp.where(mask, 1.0, 0.0).astype(BF16)

    def scale_copy(d):
        to = lax.rem(t + d, m)
        return pltpu.make_async_remote_copy(
            src_ref=sg_in.at[to], dst_ref=sct.at[0:nb2, pl.ds(al(t * kr, 128), kr)],
            send_sem=s_sc.at[0, d], recv_sem=r_sc.at[0, d], device_id={"tp": to}, device_id_type=MESH)

    def scale_down_copy(d):
        to = lax.rem(t + d, m)
        return pltpu.make_async_remote_copy(
            src_ref=sd_in.at[to], dst_ref=sd.at[:, pl.ds(al(t * dcw, 128), dcw)],
            send_sem=s_sc.at[1, d], recv_sem=r_sc.at[1, d], device_id={"tp": to}, device_id_type=MESH)

    def code_copy(c, which, d):
        src, dst = ((cg_in, cg), (cu_in, cu))[which]
        to = lax.rem(t + d, m)
        return pltpu.make_async_remote_copy(
            src_ref=src.at[:, pl.ds(al(to * units + c * cw, 128), cw)],
            dst_ref=dst.at[mine, pl.ds(al(c * cw, 128), cw)],
            send_sem=s_code.at[c, which, d], recv_sem=r_code.at[c, which, d],
            device_id={"tp": to}, device_id_type=MESH)

    def down_copy(d):
        to = lax.rem(t + d, m)
        return pltpu.make_async_remote_copy(
            src_ref=cd_in.at[pl.ds(al(to * units, 16), units), :],
            dst_ref=cd.at[:, pl.ds(al(t * dcw, 128), dcw)],
            send_sem=s_down.at[d], recv_sem=r_down.at[d],
            device_id={"tp": to}, device_id_type=MESH)

    def codes_start(c):
        for d in range(1, m):
            code_copy(c, 0, d).start()
            code_copy(c, 1, d).start()

    def normalise(b):
        for d in range(1, m):
            rows_out(b, d).wait_recv()
        values = wide[b].astype(F32)
        inverse = lax.rsqrt(jnp.mean(values * values, axis=1, keepdims=True) + EPSILON)
        normed = (values * inverse * gain_ref[...]).astype(BF16)
        for j in range(n):
            cut[b, j] = normed[:, j * depth:(j + 1) * depth]
        grp[b, pl.ds(al(f * ns, 16), ns), :] = cut[b, f]
        for d in range(1, n):
            normed_out(b, d).start()

    def gather(b):
        for d in range(1, n):
            normed_out(b, d).wait_recv()
        mine_x = jnp.zeros((rp, depth), F32)
        for g in range(n):
            place = ones_at(lax.broadcasted_iota(jnp.int32, (rp, ns), 0) == slot_index(b, g, 1))
            mine_x = mine_x + jnp.dot(place, grp[b, g * ns:(g + 1) * ns, :], preferred_element_type=F32)
        x_ref[my_part(b), :] = mine_x.astype(BF16)
        relay(b, 0)

    pl.semaphore_wait(barrier, m + n - 2)
    for d in range(1, n):
        bound_copy(d).start()
    codes_start(0)
    bounds[f] = cu_ref[...]
    for d in range(1, n):
        bound_copy(d).wait_recv()
    place_of = home_index(1)
    step = 2 * BLOCKS * ns
    for i in range(m // 2):
        spread = ones_at(lax.broadcasted_iota(jnp.int32, (step, cap), 0) + i * step == place_of)
        sent[i * step:(i + 1) * step, :] = jnp.dot(spread, tok_ref[...], preferred_element_type=F32).astype(BF16)
    for b in range(BLOCKS):
        for d in range(1, m):
            rows_out(b, d).start()
    if here:
        for d in range(1, m):
            scale_copy(d).start()
            scale_down_copy(d).start()
    for b in range(BLOCKS):
        wide[b, :, my_feat] = sent[home_rows(t, b), :]
    for b in range(BLOCKS):
        normalise(b)
    gather(0)
    local[5].wait()
    if here:
        for d in range(1, m):
            scale_copy(d).wait_recv()
    for j in range(depth // 128):
        st[j * 128:(j + 1) * 128, :] = sct[:, j * 128:(j + 1) * 128].T
    for phase in range(1, len(far_bits) + 1):
        relay(0, phase)
    ahead = min(3, chunks)
    for c in range(1, ahead):
        codes_start(c)
    local[0].wait()
    local[1].wait()

    def unpack(c):
        slot = lax.rem(c, 2)

        @pl.when(c + 1 < chunks)
        def _():
            base_start(c + 1, 1 - slot)
        base_copy(c, slot, 0, bg_in).wait()
        base_copy(c, slot, 1, bu_in).wait()
        for d in range(1, m):
            code_copy(c, 0, d).wait_recv()
            code_copy(c, 1, d).wait_recv()
        there = pl.ds(al(c * cw, 128), cw)
        scales = st[...]
        lane = lax.broadcasted_iota(jnp.int32, scales.shape, 1)
        for which, codes in ((0, cg), (1, cu)):
            picked = jnp.where(lane == c + which * chunks, scales, 0.0)
            column = jnp.sum(picked, axis=1, keepdims=True)
            codes[:, there] = (base[slot, which].astype(F32) + codes[:, there].astype(F32) * column).astype(BF16)

    def partial(k):
        b, c = k // chunks, lax.rem(k, chunks)

        @pl.when(c == 0)
        def _():
            x_wait(b)

        @pl.when(b == 0)
        def _():
            unpack(c)
        there = pl.ds(al(c * cw, 128), cw)
        both = jnp.concatenate([cg[:, there], cu[:, there]], axis=1)
        for side in range(2):
            xs = x_ref[pl.ds(al(b * rows + side * half, 16), half), :]
            own[side, k] = jnp.dot(xs, both, preferred_element_type=F32).astype(BF16)

    piece = half // SUB

    def spot(k, side, u):
        b, c = k // chunks, lax.rem(k, chunks)
        return hid.at[pl.ds(al(b * rows + side * half + u * piece, 16), piece), pl.ds(al(c * cw, 128), cw)]

    def red_copy(k, side, u):
        there = pl.ds(u * piece, piece)
        return pltpu.make_async_remote_copy(
            src_ref=own.at[side, k, there, :], dst_ref=got.at[side, k, there, :],
            send_sem=s_red.at[side, k, u], recv_sem=r_red.at[side, k, u],
            device_id={"fsdp": jnp.clip(f + (1 if side else -1), 0, last)}, device_id_type=MESH)

    def hid_copy(k, side, u):
        return pltpu.make_async_remote_copy(
            src_ref=spot(k, side, u), dst_ref=spot(k, side, u),
            send_sem=s_hid.at[side, k, u], recv_sem=r_hid.at[side, k, u],
            device_id={"fsdp": jnp.clip(f + (-1 if side else 1), 0, last)}, device_id_type=MESH)

    def valid(k):
        return (k >= 0) & (k < total)

    def reduce_step(s, side, u):
        far = f if side else last - f
        k = s - far
        there = pl.ds(u * piece, piece)

        @pl.when(valid(k) & (far > 0))
        def _():
            red_copy(k, side, u).wait_recv()

            @pl.when(far < last)
            def _():
                own[side, k, there] = (own[side, k, there].astype(F32) + got[side, k, there].astype(F32)).astype(BF16)

            @pl.when(far == last)
            def _():
                both = own[side, k, there].astype(F32) + got[side, k, there].astype(F32)
                gate, up = both[:, :cw], both[:, cw:]
                b, c = k // chunks, lax.rem(k, chunks)
                hid[pl.ds(al(b * rows + side * half + u * piece, 16), piece), pl.ds(al(c * cw, 128), cw)] = (
                    jax.nn.silu(gate) * up).astype(BF16)

    def reduce_send(s, side, u):
        far = f if side else last - f
        k = s - far

        @pl.when(valid(k) & (far < last))
        def _():
            red_copy(k, side, u).start()

        @pl.when(valid(k) & (far == last))
        def _():
            hid_copy(k, side, u).start()

    def pass_on(s, side, u):
        far = f if side else last - f
        k = s - last - (last - far)

        @pl.when(valid(k) & (far < last))
        def _():
            hid_copy(k, side, u).wait_recv()

            @pl.when(far > 0)
            def _():
                hid_copy(k, side, u).start()

    def down_weights():
        for i in range(2, 5):
            local[i].wait()
        if here:
            for d in range(1, m):
                scale_down_copy(d).wait_recv()
                down_copy(d).wait_recv()

        @pl.loop(0, chunks)
        def _(c):
            there = pl.ds(al(c * cw, 16), cw)
            cd[there, :] = (bd[there, :].astype(F32) + cd[there, :].astype(F32) * sd[pl.ds(c, 1), :]).astype(BF16)

    def down(b):
        for q in range(QUARTERS):
            block = jnp.dot(hid[pl.ds(al(b * rows, 16), rows), :], cd[:, q * dq:(q + 1) * dq],
                            preferred_element_type=F32)
            part_out[b, q] = block.astype(BF16)
            for d in range(1, m):
                sum_out(b, q, d).start()

    def send_back(b, q):
        acc = part_out[b, q, pl.ds(al(t * rp, 16), rp), :].astype(F32)
        for d in range(1, m):
            sum_out(b, q, d).wait_recv()
        for d in range(1, m):
            acc = acc + part_in[b, q, lax.rem(t + d, m)].astype(F32)
        acc = acc.astype(BF16)
        for g in range(n):
            place = ones_at(lax.broadcasted_iota(jnp.int32, (ns, rp), 1) == slot_index(b, g, 0))
            back[b, q, g] = jnp.dot(place, acc, preferred_element_type=F32).astype(BF16)
        for d in range(1, n):
            back_out(b, q, d).start()
        back_wide[b, :, quarter(q)] = back[b, q, f]

    def send_home(b, h):
        for q in range(h * per, (h + 1) * per):
            for d in range(1, n):
                back_out(b, q, d).wait_recv()
        for d in range(1, m):
            @pl.when(lax.rem(lax.rem(t + d, m), m // n) == h)
            def _():
                home_out(b, d).start()

        @pl.when(lax.rem(t, m // n) == h)
        def _():
            home[home_rows(t, b), :] = back_wide[b, :, my_feat]

    steps = total + 2 * last
    tasks = [(chunks - 1 + 2 * last, down_weights)]
    for b in range(1, BLOCKS):
        tasks.append((1, functools.partial(gather, b)))
        for phase in range(1, len(far_bits) + 1):
            tasks.append((1 + 2 * phase, functools.partial(relay, b, phase)))
    if here:
        for d in range(1, m):
            tasks.append((max(chunks - 3, 0) + d, down_copy(d).start))
    for b in range(BLOCKS):
        at = (b + 1) * chunks - 1 + 2 * last
        tasks.append((at, functools.partial(down, b)))
        for q in range(QUARTERS):
            tasks.append((at + 3 + q // 2, functools.partial(send_back, b, q)))
            if q % per == per - 1:
                tasks.append((at + 5 + q // 2, functools.partial(send_home, b, q // per)))

    partial(0)

    @pl.loop(0, steps)
    def _(s):
        for u in range(SUB):
            for side in range(2):
                reduce_step(s, side, u)
            for side in range(2):
                reduce_send(s, side, u)
        for u in range(SUB):
            for side in range(2):
                pass_on(s, side, u)

        @pl.when(s + ahead < chunks)
        def _():
            codes_start(s + ahead)

        @pl.when(s + 1 < total)
        def _():
            partial(s + 1)
        for at, task in tasks:
            if at < steps:
                pl.when(s == at)(task)

    late = [task for at, task in tasks if at >= steps]
    for task in late:
        task()
    for b in range(BLOCKS):
        for d in range(1, m):
            home_out(b, d).wait_recv()
    place_of = home_index(0)
    for i in range(0, cap, 256):
        stop = min(i + 256, cap)
        spread = ones_at(lax.broadcasted_iota(jnp.int32, (stop - i, m * BLOCKS * ns), 1) == place_of[i:stop])
        out_ref[i:stop, :] = jnp.dot(spread, home[...], preferred_element_type=F32).astype(BF16)

    @pl.loop(0, chunks)
    def _(c):
        for d in range(1, m):
            code_copy(c, 0, d).wait_send()
            code_copy(c, 1, d).wait_send()
    if here:
        for d in range(1, m):
            down_copy(d).wait_send()
            scale_copy(d).wait_send()
            scale_down_copy(d).wait_send()
    for b in range(BLOCKS):
        for d in range(1, m):
            for out in (rows_out, home_out):
                out(b, d).wait_send()
            for q in range(QUARTERS):
                sum_out(b, q, d).wait_send()
        x_sent(b)
        for d in range(1, n):
            normed_out(b, d).wait_send()
            for q in range(QUARTERS):
                back_out(b, q, d).wait_send()

    for d in range(1, n):
        bound_copy(d).wait_send()

    @pl.loop(0, total)
    def _(k):
        for side in range(2):
            far = f if side else last - f

            @pl.when(far < last)
            def _():
                for u in range(SUB):
                    red_copy(k, side, u).wait_send()

            @pl.when(far > 0)
            def _():
                for u in range(SUB):
                    hid_copy(k, side, u).wait_send()


def layer(n, m, here, tokens, gain, cu_seqlens, code_gate, code_up, scales, base_gate, base_up,
          code_down, scale_down, base_down):
    width, units = base_gate.shape
    depth = width // n
    cap, feat = tokens.shape
    live_all = n * (cap // 2 + SEQS)
    ns = -(-(-(-cap // (BLOCKS * m))) // 16) * 16
    chunks = scale_down.shape[-2]
    cw = units // chunks
    total = BLOCKS * chunks
    half = live_all // (2 * BLOCKS)
    rp = live_all // (BLOCKS * m)
    dq = depth // QUARTERS
    anywhere = pl.BlockSpec(memory_space=pl.ANY)
    near = pl.BlockSpec(memory_space=pltpu.VMEM)
    dma = pltpu.SemaphoreType.DMA
    vm = pltpu.VMEM
    return pl.pallas_call(
        functools.partial(layer_kernel, n, m, here),
        out_shape=jax.ShapeDtypeStruct((cap, feat), BF16),
        in_specs=[near, near, near] + [anywhere] * 8,
        out_specs=near,
        scratch_shapes=[
            vm((depth, units), BF16), vm((depth, units), BF16), vm((2, 2, depth, cw), BF16),
            vm((2, total, half, 2 * cw), BF16), vm((2, total, half, 2 * cw), BF16),
            vm((live_all, units), BF16), vm((units, depth), BF16), vm((units, depth), BF16),
            vm((live_all, depth), BF16), vm((BLOCKS, ns, width), BF16), vm((BLOCKS, n, ns, depth), BF16),
            vm((BLOCKS, n * ns, depth), BF16), vm((BLOCKS, QUARTERS, m * rp, dq), BF16),
            vm((BLOCKS, QUARTERS, m, rp, dq), BF16), vm((BLOCKS, QUARTERS, n, ns, dq), BF16),
            vm((BLOCKS, ns, width), BF16),
            vm((depth, 128), F32), vm((128, depth), F32), vm((chunks, depth), F32),
            vm((m * BLOCKS * ns, feat), BF16), vm((m * BLOCKS * ns, feat), BF16), vm((n,) + cu_seqlens.shape, jnp.int32),
            dma((chunks, 2, m)), dma((chunks, 2, m)), dma((m,)), dma((m,)), dma((6,)), dma((2, 2)),
            dma((2, total, SUB)), dma((2, total, SUB)), dma((2, total, SUB)), dma((2, total, SUB)),
            dma((BLOCKS, 2, m)), dma((BLOCKS, 2, m)),
            dma((2, BLOCKS, m)), dma((2, BLOCKS, m)), dma((1, BLOCKS, n)), dma((1, BLOCKS, n)), dma((2, m)), dma((2, m)),
            dma((BLOCKS, QUARTERS, m)), dma((BLOCKS, QUARTERS, m)), dma((BLOCKS, QUARTERS, n)), dma((BLOCKS, QUARTERS, n)),
            dma((n,)), dma((n,)),
        ],
        compiler_params=pltpu.CompilerParams(
            collective_id=0, has_side_effects=True, vmem_limit_bytes=67043328),
    )(tokens, gain, cu_seqlens, code_gate, code_up, scales, base_gate, base_up, code_down, scale_down, base_down)


def shards(tokens, norm_gain, base_gate, base_up, base_down, code_gate, code_up,
           scale_gate, scale_up, code_down, scale_down, cu_seqlens):
    n, m = lax.axis_size("fsdp"), lax.axis_size("tp")
    kr = code_gate.shape[0]
    nb = scale_gate.shape[1] // m
    scales = jnp.concatenate([scale_gate.reshape(kr, m, nb), scale_up.reshape(kr, m, nb)], axis=2).transpose(1, 2, 0)
    scales = jnp.pad(scales, ((0, 0), (0, -(2 * nb) % 8), (0, 0)))
    scale_down = scale_down.reshape(m, nb, -1)
    here = code_down.shape[1] % 128 == 0 and kr % 128 == 0
    if not here:
        code_down = lax.all_to_all(code_down, "tp", split_axis=0, concat_axis=1, tiled=True)
        scales = lax.all_to_all(scales, "tp", split_axis=0, concat_axis=2, tiled=True)[0]
        scale_down = lax.all_to_all(scale_down, "tp", split_axis=0, concat_axis=2, tiled=True)[0]
    summed_out = layer(n, m, here, tokens, norm_gain[None, :], cu_seqlens, code_gate, code_up, scales,
                       base_gate, base_up, code_down, scale_down, base_down)

    bounds = cu_seqlens[0]
    slots = jnp.arange(tokens.shape[0], dtype=jnp.int32)
    mixed = (tokens.astype(F32) + summed_out.astype(F32)).astype(BF16)
    mixed = jnp.where((slots < bounds[SEQS])[:, None], mixed, jnp.zeros((), BF16))
    member = (slots[None, :] >= bounds[:-1, None]) & (slots[None, :] < bounds[1:, None])
    seq_sums = jnp.dot(member.astype(BF16), mixed, preferred_element_type=F32)
    lengths = (bounds[1:] - bounds[:-1]).astype(F32)
    return mixed, seq_sums / lengths[:, None]


def solution(mesh):
    placed = (
        P("fsdp", "tp"), P(), P(None, "tp"), P(None, "tp"), P("tp", None),
        P(("fsdp", "tp"), None), P(("fsdp", "tp"), None),
        P(("fsdp", "tp"), None), P(("fsdp", "tp"), None),
        P(None, ("fsdp", "tp")), P(None, ("fsdp", "tp")), P("fsdp", None),
    )
    return jax.shard_map(shards, mesh=mesh, in_specs=placed,
                         out_specs=(P("fsdp", "tp"), P("fsdp", "tp")), check_vma=False)
```

```python
import functools
import jax
import jax.numpy as jnp
from jax import lax
from jax.experimental import pallas as pl
from jax.experimental.pallas import tpu as pltpu
from jax.sharding import PartitionSpec as P

SEQS = 8
EPSILON = 1e-06
BLOCKS = 2
SUB = 2
QUARTERS = 2
F32, BF16 = jnp.float32, jnp.bfloat16
MESH = pl.DeviceIdType.MESH


def al(value, size):
    return pl.multiple_of(value, size)


def layer_kernel(n, m, here, *refs):
    (tok_ref, gain_ref, cu_ref, cg_in, cu_in, sg_in, bg_in, bu_in, cd_in, sd_in, bd_in, out_ref, mean_ref,
     cg, cu, base, own, got, hid, cd, bd, x_ref, wide, cut, grp, part_out, part_in, back, back_wide, st, sct, sd,
     sent, home, bounds,
     s_code, r_code, s_down, r_down, l_sem, b_sem, s_red, r_red, s_hid, r_hid, s_x, r_x,
     s_tp, r_tp, s_fs, r_fs, s_sc, r_sc, s_sum, r_sum, s_back, r_back, s_bound, r_bound) = refs
    f, t = lax.axis_index("fsdp"), lax.axis_index("tp")
    kr = cg_in.shape[0]
    depth, units = cg.shape
    cw = base.shape[3]
    chunks = units // cw
    rows = x_ref.shape[0] // BLOCKS
    half = rows // 2
    rp = rows // m
    cap, feat = tok_ref.shape
    ns = wide.shape[1]
    lanes = BLOCKS * m
    lane_bits, part_bits = lanes.bit_length() - 1, m.bit_length() - 1
    dq = depth // QUARTERS
    per = QUARTERS // (m // n)
    nb2 = sg_in.shape[-2]
    total = BLOCKS * chunks
    last = n - 1
    dcw = depth // m

    barrier = pltpu.get_barrier_semaphore()
    for d in range(1, m):
        pl.semaphore_signal(barrier, inc=1, device_id={"tp": lax.rem(t + d, m)}, device_id_type=MESH)
    for d in range(1, n):
        pl.semaphore_signal(barrier, inc=1, device_id={"fsdp": lax.rem(f + d, n)}, device_id_type=MESH)

    def base_copy(c, slot, which, src):
        return pltpu.make_async_copy(
            src.at[pl.ds(al(f * depth, 16), depth), pl.ds(al(c * cw, 128), cw)],
            base.at[slot, which], b_sem.at[slot, which])

    def base_start(c, slot):
        base_copy(c, slot, 0, bg_in).start()
        base_copy(c, slot, 1, bu_in).start()

    mine = pl.ds(al(t * kr, 16), kr)
    cols = pl.ds(al(t * units, 128), units)
    local = [pltpu.make_async_copy(cg_in.at[:, cols], cg.at[mine, :], l_sem.at[0]),
             pltpu.make_async_copy(cu_in.at[:, cols], cu.at[mine, :], l_sem.at[1]),
             pltpu.make_async_copy(bd_in.at[:, pl.ds(al(f * depth, 128), depth)], bd, l_sem.at[2])]
    if here:
        local += [pltpu.make_async_copy(
            cd_in.at[pl.ds(al(t * units, 16), units), :], cd.at[:, pl.ds(al(t * dcw, 128), dcw)], l_sem.at[3]),
            pltpu.make_async_copy(sd_in.at[t], sd.at[:, pl.ds(al(t * dcw, 128), dcw)], l_sem.at[4]),
            pltpu.make_async_copy(sg_in.at[t], sct.at[0:nb2, pl.ds(al(t * kr, 128), kr)], l_sem.at[5])]
    else:
        local += [pltpu.make_async_copy(cd_in, cd, l_sem.at[3]), pltpu.make_async_copy(sd_in, sd, l_sem.at[4]),
                  pltpu.make_async_copy(sg_in, sct.at[0:nb2, :], l_sem.at[5])]
    base_start(0, 0)
    if nb2 < sct.shape[0]:
        sct[nb2:, :] = jnp.zeros_like(sct[nb2:, :])
    for copy in local:
        copy.start()

    def to_tp(b, stage, d, src, dst):
        return pltpu.make_async_remote_copy(
            src_ref=src, dst_ref=dst, send_sem=s_tp.at[stage, b, d], recv_sem=r_tp.at[stage, b, d],
            device_id={"tp": lax.rem(t + d, m)}, device_id_type=MESH)

    def to_fs(b, stage, d, src, dst):
        return pltpu.make_async_remote_copy(
            src_ref=src, dst_ref=dst, send_sem=s_fs.at[stage, b, d], recv_sem=r_fs.at[stage, b, d],
            device_id={"fsdp": lax.rem(f + d, n)}, device_id_type=MESH)

    my_feat = pl.ds(al(t * feat, 128), feat)
    my_depth = pl.ds(al(f * depth, 128), depth)

    def my_part(b):
        return pl.ds(al(b * rows + t * rp, 16), rp)

    def home_rows(part, b):
        return pl.ds(al((part * BLOCKS + b) * ns, 16), ns)

    def rows_out(b, d):
        return to_tp(b, 0, d, sent.at[home_rows(lax.rem(t + d, m), b), :], wide.at[b, :, my_feat])

    def normed_out(b, d):
        return to_fs(b, 0, d, cut.at[b, lax.rem(f + d, n)], grp.at[b, pl.ds(al(f * ns, 16), ns), :])

    def flip(bits):
        peer, bit = t, 1
        while bit <= bits:
            if bits & bit:
                peer = peer + bit - 2 * bit * lax.rem(t // bit, 2)
            bit *= 2
        return peer

    def x_copy(b, h, mask, bit):
        spot = x_ref.at[pl.ds(al(b * rows + flip(mask) * rp + h * (rp // 2), 16), rp // 2), :]
        return pltpu.make_async_remote_copy(
            src_ref=spot, dst_ref=spot, send_sem=s_x.at[b, h, mask ^ bit], recv_sem=r_x.at[b, h, mask ^ bit],
            device_id={"tp": flip(bit)}, device_id_type=MESH)

    def x_arrived(b, h, mask):
        spot = x_ref.at[pl.ds(al(b * rows + flip(mask) * rp + h * (rp // 2), 16), rp // 2), :]
        pltpu.make_async_remote_copy(
            src_ref=spot, dst_ref=spot, send_sem=s_x.at[b, h, mask], recv_sem=r_x.at[b, h, mask],
            device_id={"tp": flip(1)}, device_id_type=MESH).wait_recv()

    far_bits = [2 ** i for i in range(1, m.bit_length() - 1)]
    far_masks = sorted(range(2, m, 2), key=lambda mask: (bin(mask).count("1"), mask))
    orders = (far_bits, far_bits[::-1])

    def onward(h, mask):
        order = orders[h]
        used = [i for i, bit in enumerate(order) if mask & bit]
        return order[max(used, default=-1) + 1:]

    def relay(b, phase):
        for mask in [0] + far_masks:
            if bin(mask).count("1") == phase:
                for h in range(2):
                    if mask:
                        x_arrived(b, h, mask)
                    for bit in onward(h, mask) + [1]:
                        x_copy(b, h, mask, bit).start()

    def x_wait(b):
        for mask in range(1, m, 2):
            for h in range(2):
                x_arrived(b, h, mask)

    def x_sent(b):
        for mask in [0] + far_masks:
            for h in range(2):
                for bit in onward(h, mask) + [1]:
                    x_copy(b, h, mask, bit).wait_send()

    def sum_out(b, q, d):
        return pltpu.make_async_remote_copy(
            src_ref=part_out.at[b, q, pl.ds(al(lax.rem(t + d, m) * rp, 16), rp), :], dst_ref=part_in.at[b, q, t],
            send_sem=s_sum.at[b, q, d], recv_sem=r_sum.at[b, q, d],
            device_id={"tp": lax.rem(t + d, m)}, device_id_type=MESH)

    def quarter(q):
        return pl.ds(al(f * depth + q * dq, 128), dq)

    def back_out(b, q, d):
        return pltpu.make_async_remote_copy(
            src_ref=back.at[b, q, lax.rem(f + d, n)], dst_ref=back_wide.at[b, :, quarter(q)],
            send_sem=s_back.at[b, q, d], recv_sem=r_back.at[b, q, d],
            device_id={"fsdp": lax.rem(f + d, n)}, device_id_type=MESH)

    def home_out(b, d):
        return to_tp(b, 1, d, back_wide.at[b, :, pl.ds(al(lax.rem(t + d, m) * feat, 128), feat)],
                     home.at[home_rows(t, b), :])

    def bound_copy(d):
        return pltpu.make_async_remote_copy(
            src_ref=cu_ref, dst_ref=bounds.at[f], send_sem=s_bound.at[d], recv_sem=r_bound.at[d],
            device_id={"fsdp": lax.rem(f + d, n)}, device_id_type=MESH)

    def group_counts():
        counts = [bounds[g][:, SEQS:SEQS + 1] for g in range(n)]
        starts = [jnp.zeros_like(counts[0])]
        for g in range(1, n):
            starts.append(starts[-1] + counts[g - 1])
        return starts, counts

    def home_index(axis):
        starts, counts = group_counts()
        start = sum(jnp.where(f == g, starts[g], 0) for g in range(n))
        live = sum(jnp.where(f == g, counts[g], 0) for g in range(n))
        shape = (cap, 1) if axis == 0 else (1, cap)
        r = lax.broadcasted_iota(jnp.int32, shape, axis)
        lane = (r + start) & (lanes - 1)
        index = ((lane & (m - 1)) * BLOCKS + (lane >> part_bits)) * ns + (r >> lane_bits)
        return jnp.where(r < live, index, -1)

    def slot_index(b, g, axis):
        starts, counts = group_counts()
        shape = (ns, 1) if axis == 0 else (1, ns)
        r = ((t + m * b - starts[g]) & (lanes - 1)) + lanes * lax.broadcasted_iota(jnp.int32, shape, axis)
        return jnp.where(r < counts[g], (starts[g] + r) >> lane_bits, -1)

    def ones_at(mask):
        return jnp.where(mask, 1.0, 0.0).astype(BF16)

    def scale_copy(d):
        to = lax.rem(t + d, m)
        return pltpu.make_async_remote_copy(
            src_ref=sg_in.at[to], dst_ref=sct.at[0:nb2, pl.ds(al(t * kr, 128), kr)],
            send_sem=s_sc.at[0, d], recv_sem=r_sc.at[0, d], device_id={"tp": to}, device_id_type=MESH)

    def scale_down_copy(d):
        to = lax.rem(t + d, m)
        return pltpu.make_async_remote_copy(
            src_ref=sd_in.at[to], dst_ref=sd.at[:, pl.ds(al(t * dcw, 128), dcw)],
            send_sem=s_sc.at[1, d], recv_sem=r_sc.at[1, d], device_id={"tp": to}, device_id_type=MESH)

    def code_copy(c, which, d):
        src, dst = ((cg_in, cg), (cu_in, cu))[which]
        to = lax.rem(t + d, m)
        return pltpu.make_async_remote_copy(
            src_ref=src.at[:, pl.ds(al(to * units + c * cw, 128), cw)],
            dst_ref=dst.at[mine, pl.ds(al(c * cw, 128), cw)],
            send_sem=s_code.at[c, which, d], recv_sem=r_code.at[c, which, d],
            device_id={"tp": to}, device_id_type=MESH)

    def down_copy(d):
        to = lax.rem(t + d, m)
        return pltpu.make_async_remote_copy(
            src_ref=cd_in.at[pl.ds(al(to * units, 16), units), :],
            dst_ref=cd.at[:, pl.ds(al(t * dcw, 128), dcw)],
            send_sem=s_down.at[d], recv_sem=r_down.at[d],
            device_id={"tp": to}, device_id_type=MESH)

    def codes_start(c):
        for d in range(1, m):
            code_copy(c, 0, d).start()
            code_copy(c, 1, d).start()

    def normalise(b):
        for d in range(1, m):
            rows_out(b, d).wait_recv()
        values = wide[b].astype(F32)
        inverse = lax.rsqrt(jnp.mean(values * values, axis=1, keepdims=True) + EPSILON)
        normed = (values * inverse * gain_ref[...]).astype(BF16)
        for j in range(n):
            cut[b, j] = normed[:, j * depth:(j + 1) * depth]
        grp[b, pl.ds(al(f * ns, 16), ns), :] = cut[b, f]
        for d in range(1, n):
            normed_out(b, d).start()

    def gather(b):
        for d in range(1, n):
            normed_out(b, d).wait_recv()
        mine_x = jnp.zeros((rp, depth), F32)
        for g in range(n):
            place = ones_at(lax.broadcasted_iota(jnp.int32, (rp, ns), 0) == slot_index(b, g, 1))
            mine_x = mine_x + jnp.dot(place, grp[b, g * ns:(g + 1) * ns, :], preferred_element_type=F32)
        x_ref[my_part(b), :] = mine_x.astype(BF16)
        relay(b, 0)

    pl.semaphore_wait(barrier, m + n - 2)
    for d in range(1, n):
        bound_copy(d).start()
    codes_start(0)
    bounds[f] = cu_ref[...]
    for d in range(1, n):
        bound_copy(d).wait_recv()
    place_of = home_index(1)
    step = 2 * BLOCKS * ns
    for i in range(m // 2):
        spread = ones_at(lax.broadcasted_iota(jnp.int32, (step, cap), 0) + i * step == place_of)
        sent[i * step:(i + 1) * step, :] = jnp.dot(spread, tok_ref[...], preferred_element_type=F32).astype(BF16)
    for b in range(BLOCKS):
        for d in range(1, m):
            rows_out(b, d).start()
    if here:
        for d in range(1, m):
            scale_copy(d).start()
            scale_down_copy(d).start()
    for b in range(BLOCKS):
        wide[b, :, my_feat] = sent[home_rows(t, b), :]
    for b in range(BLOCKS):
        normalise(b)
    gather(0)
    local[5].wait()
    if here:
        for d in range(1, m):
            scale_copy(d).wait_recv()
    for j in range(depth // 128):
        st[j * 128:(j + 1) * 128, :] = sct[:, j * 128:(j + 1) * 128].T
    for phase in range(1, len(far_bits) + 1):
        relay(0, phase)
    ahead = min(3, chunks)
    for c in range(1, ahead):
        codes_start(c)
    local[0].wait()
    local[1].wait()

    def unpack(c):
        slot = lax.rem(c, 2)

        @pl.when(c + 1 < chunks)
        def _():
            base_start(c + 1, 1 - slot)
        base_copy(c, slot, 0, bg_in).wait()
        base_copy(c, slot, 1, bu_in).wait()
        for d in range(1, m):
            code_copy(c, 0, d).wait_recv()
            code_copy(c, 1, d).wait_recv()
        there = pl.ds(al(c * cw, 128), cw)
        scales = st[...]
        lane = lax.broadcasted_iota(jnp.int32, scales.shape, 1)
        for which, codes in ((0, cg), (1, cu)):
            picked = jnp.where(lane == c + which * chunks, scales, 0.0)
            column = jnp.sum(picked, axis=1, keepdims=True)
            codes[:, there] = (base[slot, which].astype(F32) + codes[:, there].astype(F32) * column).astype(BF16)

    def partial(k):
        b, c = k // chunks, lax.rem(k, chunks)

        @pl.when(c == 0)
        def _():
            x_wait(b)

        @pl.when(b == 0)
        def _():
            unpack(c)
        there = pl.ds(al(c * cw, 128), cw)
        both = jnp.concatenate([cg[:, there], cu[:, there]], axis=1)
        for side in range(2):
            xs = x_ref[pl.ds(al(b * rows + side * half, 16), half), :]
            own[side, k] = jnp.dot(xs, both, preferred_element_type=F32).astype(BF16)

    piece = half // SUB

    def spot(k, side, u):
        b, c = k // chunks, lax.rem(k, chunks)
        return hid.at[pl.ds(al(b * rows + side * half + u * piece, 16), piece), pl.ds(al(c * cw, 128), cw)]

    def red_copy(k, side, u):
        there = pl.ds(u * piece, piece)
        return pltpu.make_async_remote_copy(
            src_ref=own.at[side, k, there, :], dst_ref=got.at[side, k, there, :],
            send_sem=s_red.at[side, k, u], recv_sem=r_red.at[side, k, u],
            device_id={"fsdp": jnp.clip(f + (1 if side else -1), 0, last)}, device_id_type=MESH)

    def hid_copy(k, side, u):
        return pltpu.make_async_remote_copy(
            src_ref=spot(k, side, u), dst_ref=spot(k, side, u),
            send_sem=s_hid.at[side, k, u], recv_sem=r_hid.at[side, k, u],
            device_id={"fsdp": jnp.clip(f + (-1 if side else 1), 0, last)}, device_id_type=MESH)

    def valid(k):
        return (k >= 0) & (k < total)

    def reduce_step(s, side, u):
        far = f if side else last - f
        k = s - far
        there = pl.ds(u * piece, piece)

        @pl.when(valid(k) & (far > 0))
        def _():
            red_copy(k, side, u).wait_recv()

            @pl.when(far < last)
            def _():
                own[side, k, there] = (own[side, k, there].astype(F32) + got[side, k, there].astype(F32)).astype(BF16)

            @pl.when(far == last)
            def _():
                both = own[side, k, there].astype(F32) + got[side, k, there].astype(F32)
                gate, up = both[:, :cw], both[:, cw:]
                b, c = k // chunks, lax.rem(k, chunks)
                hid[pl.ds(al(b * rows + side * half + u * piece, 16), piece), pl.ds(al(c * cw, 128), cw)] = (
                    jax.nn.silu(gate) * up).astype(BF16)

    def reduce_send(s, side, u):
        far = f if side else last - f
        k = s - far

        @pl.when(valid(k) & (far < last))
        def _():
            red_copy(k, side, u).start()

        @pl.when(valid(k) & (far == last))
        def _():
            hid_copy(k, side, u).start()

    def pass_on(s, side, u):
        far = f if side else last - f
        k = s - last - (last - far)

        @pl.when(valid(k) & (far < last))
        def _():
            hid_copy(k, side, u).wait_recv()

            @pl.when(far > 0)
            def _():
                hid_copy(k, side, u).start()

    def down_weights():
        for i in range(2, 5):
            local[i].wait()
        if here:
            for d in range(1, m):
                scale_down_copy(d).wait_recv()
                down_copy(d).wait_recv()

        @pl.loop(0, chunks)
        def _(c):
            there = pl.ds(al(c * cw, 16), cw)
            cd[there, :] = (bd[there, :].astype(F32) + cd[there, :].astype(F32) * sd[pl.ds(c, 1), :]).astype(BF16)

    def down(b):
        for q in range(QUARTERS):
            block = jnp.dot(hid[pl.ds(al(b * rows, 16), rows), :], cd[:, q * dq:(q + 1) * dq],
                            preferred_element_type=F32)
            part_out[b, q] = block.astype(BF16)
            for d in range(1, m):
                sum_out(b, q, d).start()

    def send_back(b, q):
        acc = part_out[b, q, pl.ds(al(t * rp, 16), rp), :].astype(F32)
        for d in range(1, m):
            sum_out(b, q, d).wait_recv()
        for d in range(1, m):
            acc = acc + part_in[b, q, lax.rem(t + d, m)].astype(F32)
        acc = acc.astype(BF16)
        for g in range(n):
            place = ones_at(lax.broadcasted_iota(jnp.int32, (ns, rp), 1) == slot_index(b, g, 0))
            back[b, q, g] = jnp.dot(place, acc, preferred_element_type=F32).astype(BF16)
        for d in range(1, n):
            back_out(b, q, d).start()
        back_wide[b, :, quarter(q)] = back[b, q, f]

    def send_home(b, h):
        for q in range(h * per, (h + 1) * per):
            for d in range(1, n):
                back_out(b, q, d).wait_recv()
        for d in range(1, m):
            @pl.when(lax.rem(lax.rem(t + d, m), m // n) == h)
            def _():
                home_out(b, d).start()

        @pl.when(lax.rem(t, m // n) == h)
        def _():
            home[home_rows(t, b), :] = back_wide[b, :, my_feat]

    steps = total + 2 * last
    tasks = [(chunks - 1 + 2 * last, down_weights)]
    for b in range(1, BLOCKS):
        tasks.append((1, functools.partial(gather, b)))
        for phase in range(1, len(far_bits) + 1):
            tasks.append((1 + 2 * phase, functools.partial(relay, b, phase)))
    if here:
        for d in range(1, m):
            tasks.append((max(chunks - 3, 0) + d, down_copy(d).start))
    for b in range(BLOCKS):
        at = (b + 1) * chunks - 1 + 2 * last
        tasks.append((at, functools.partial(down, b)))
        for q in range(QUARTERS):
            tasks.append((at + 3 + q // 2, functools.partial(send_back, b, q)))
            if q % per == per - 1:
                tasks.append((at + 5 + q // 2, functools.partial(send_home, b, q // per)))

    partial(0)

    @pl.loop(0, steps)
    def _(s):
        for u in range(SUB):
            for side in range(2):
                reduce_step(s, side, u)
            for side in range(2):
                reduce_send(s, side, u)
        for u in range(SUB):
            for side in range(2):
                pass_on(s, side, u)

        @pl.when(s + ahead < chunks)
        def _():
            codes_start(s + ahead)

        @pl.when(s + 1 < total)
        def _():
            partial(s + 1)
        for at, task in tasks:
            if at < steps:
                pl.when(s == at)(task)

    late = [task for at, task in tasks if at >= steps]
    for task in late:
        task()
    for b in range(BLOCKS):
        for d in range(1, m):
            home_out(b, d).wait_recv()
    place_of = home_index(0)
    for i in range(0, cap, 256):
        stop = min(i + 256, cap)
        spread = ones_at(lax.broadcasted_iota(jnp.int32, (stop - i, m * BLOCKS * ns), 1) == place_of[i:stop])
        summed = jnp.dot(spread, home[...], preferred_element_type=F32)
        mixed = (tok_ref[i:stop, :].astype(F32) + summed).astype(BF16).astype(F32)
        out_ref[i:stop, :] = jnp.where(place_of[i:stop] >= 0, mixed, 0.0).astype(BF16)
    seq = lax.broadcasted_iota(jnp.int32, (SEQS, 1), 0)
    low = sum(jnp.where(seq == j, cu_ref[:, j:j + 1], 0) for j in range(SEQS))
    high = sum(jnp.where(seq == j, cu_ref[:, j + 1:j + 2], 0) for j in range(SEQS))
    row = lax.broadcasted_iota(jnp.int32, (SEQS, cap), 1)
    member = ones_at((row >= low) & (row < high))
    mean_ref[...] = jnp.dot(member, out_ref[...], preferred_element_type=F32) / (high - low).astype(F32)

    @pl.loop(0, chunks)
    def _(c):
        for d in range(1, m):
            code_copy(c, 0, d).wait_send()
            code_copy(c, 1, d).wait_send()
    if here:
        for d in range(1, m):
            down_copy(d).wait_send()
            scale_copy(d).wait_send()
            scale_down_copy(d).wait_send()
    for b in range(BLOCKS):
        for d in range(1, m):
            for out in (rows_out, home_out):
                out(b, d).wait_send()
            for q in range(QUARTERS):
                sum_out(b, q, d).wait_send()
        x_sent(b)
        for d in range(1, n):
            normed_out(b, d).wait_send()
            for q in range(QUARTERS):
                back_out(b, q, d).wait_send()

    for d in range(1, n):
        bound_copy(d).wait_send()

    @pl.loop(0, total)
    def _(k):
        for side in range(2):
            far = f if side else last - f

            @pl.when(far < last)
            def _():
                for u in range(SUB):
                    red_copy(k, side, u).wait_send()

            @pl.when(far > 0)
            def _():
                for u in range(SUB):
                    hid_copy(k, side, u).wait_send()


def layer(n, m, here, tokens, gain, cu_seqlens, code_gate, code_up, scales, base_gate, base_up,
          code_down, scale_down, base_down):
    width, units = base_gate.shape
    depth = width // n
    cap, feat = tokens.shape
    live_all = n * (cap // 2 + SEQS)
    ns = -(-(-(-cap // (BLOCKS * m))) // 16) * 16
    chunks = scale_down.shape[-2]
    cw = units // chunks
    total = BLOCKS * chunks
    half = live_all // (2 * BLOCKS)
    rp = live_all // (BLOCKS * m)
    dq = depth // QUARTERS
    anywhere = pl.BlockSpec(memory_space=pl.ANY)
    near = pl.BlockSpec(memory_space=pltpu.VMEM)
    dma = pltpu.SemaphoreType.DMA
    vm = pltpu.VMEM
    return pl.pallas_call(
        functools.partial(layer_kernel, n, m, here),
        out_shape=(jax.ShapeDtypeStruct((cap, feat), BF16), jax.ShapeDtypeStruct((SEQS, feat), F32)),
        in_specs=[near, near, near] + [anywhere] * 8,
        out_specs=(near, near),
        scratch_shapes=[
            vm((depth, units), BF16), vm((depth, units), BF16), vm((2, 2, depth, cw), BF16),
            vm((2, total, half, 2 * cw), BF16), vm((2, total, half, 2 * cw), BF16),
            vm((live_all, units), BF16), vm((units, depth), BF16), vm((units, depth), BF16),
            vm((live_all, depth), BF16), vm((BLOCKS, ns, width), BF16), vm((BLOCKS, n, ns, depth), BF16),
            vm((BLOCKS, n * ns, depth), BF16), vm((BLOCKS, QUARTERS, m * rp, dq), BF16),
            vm((BLOCKS, QUARTERS, m, rp, dq), BF16), vm((BLOCKS, QUARTERS, n, ns, dq), BF16),
            vm((BLOCKS, ns, width), BF16),
            vm((depth, 128), F32), vm((128, depth), F32), vm((chunks, depth), F32),
            vm((m * BLOCKS * ns, feat), BF16), vm((m * BLOCKS * ns, feat), BF16), vm((n,) + cu_seqlens.shape, jnp.int32),
            dma((chunks, 2, m)), dma((chunks, 2, m)), dma((m,)), dma((m,)), dma((6,)), dma((2, 2)),
            dma((2, total, SUB)), dma((2, total, SUB)), dma((2, total, SUB)), dma((2, total, SUB)),
            dma((BLOCKS, 2, m)), dma((BLOCKS, 2, m)),
            dma((2, BLOCKS, m)), dma((2, BLOCKS, m)), dma((1, BLOCKS, n)), dma((1, BLOCKS, n)), dma((2, m)), dma((2, m)),
            dma((BLOCKS, QUARTERS, m)), dma((BLOCKS, QUARTERS, m)), dma((BLOCKS, QUARTERS, n)), dma((BLOCKS, QUARTERS, n)),
            dma((n,)), dma((n,)),
        ],
        compiler_params=pltpu.CompilerParams(
            collective_id=0, has_side_effects=True, vmem_limit_bytes=67043328),
    )(tokens, gain, cu_seqlens, code_gate, code_up, scales, base_gate, base_up, code_down, scale_down, base_down)


def shards(tokens, norm_gain, base_gate, base_up, base_down, code_gate, code_up,
           scale_gate, scale_up, code_down, scale_down, cu_seqlens):
    n, m = lax.axis_size("fsdp"), lax.axis_size("tp")
    kr = code_gate.shape[0]
    nb = scale_gate.shape[1] // m
    scales = jnp.concatenate([scale_gate.reshape(kr, m, nb), scale_up.reshape(kr, m, nb)], axis=2).transpose(1, 2, 0)
    scales = jnp.pad(scales, ((0, 0), (0, -(2 * nb) % 8), (0, 0)))
    scale_down = scale_down.reshape(m, nb, -1)
    here = code_down.shape[1] % 128 == 0 and kr % 128 == 0
    if not here:
        code_down = lax.all_to_all(code_down, "tp", split_axis=0, concat_axis=1, tiled=True)
        scales = lax.all_to_all(scales, "tp", split_axis=0, concat_axis=2, tiled=True)[0]
        scale_down = lax.all_to_all(scale_down, "tp", split_axis=0, concat_axis=2, tiled=True)[0]
    return layer(n, m, here, tokens, norm_gain[None, :], cu_seqlens, code_gate, code_up, scales,
                 base_gate, base_up, code_down, scale_down, base_down)


def solution(mesh):
    placed = (
        P("fsdp", "tp"), P(), P(None, "tp"), P(None, "tp"), P("tp", None),
        P(("fsdp", "tp"), None), P(("fsdp", "tp"), None),
        P(("fsdp", "tp"), None), P(("fsdp", "tp"), None),
        P(None, ("fsdp", "tp")), P(None, ("fsdp", "tp")), P("fsdp", None),
    )
    return jax.shard_map(shards, mesh=mesh, in_specs=placed,
                         out_specs=(P("fsdp", "tp"), P("fsdp", "tp")), check_vma=False)
```

```python
import functools
import jax
import jax.numpy as jnp
from jax import lax
from jax.experimental import pallas as pl
from jax.experimental.pallas import tpu as pltpu
from jax.sharding import PartitionSpec as P

SEQS = 8
EPSILON = 1e-06
BLOCKS = 2
SUB = 2
QUARTERS = 2
F32, BF16 = jnp.float32, jnp.bfloat16
MESH = pl.DeviceIdType.MESH


def al(value, size):
    return pl.multiple_of(value, size)


def layer_kernel(n, m, here, *refs):
    (tok_ref, gain_ref, cu_ref, cg_in, cu_in, sg_in, bg_in, bu_in, cd_in, sd_in, bd_in, out_ref, mean_ref,
     cg, cu, base, own, got, hid, cd, bd, x_ref, wide, cut, grp, part_out, part_in, back, back_wide, st, sct, sd,
     sent, home, bounds,
     s_code, r_code, s_down, r_down, l_sem, b_sem, s_red, r_red, s_hid, r_hid, s_x, r_x,
     s_tp, r_tp, s_fs, r_fs, s_sc, r_sc, s_sum, r_sum, s_back, r_back, s_bound, r_bound) = refs
    f, t = lax.axis_index("fsdp"), lax.axis_index("tp")
    kr = cg_in.shape[0]
    depth, units = cg.shape
    cw = base.shape[3]
    chunks = units // cw
    rows = x_ref.shape[0] // BLOCKS
    half = rows // 2
    rp = rows // m
    cap, feat = tok_ref.shape
    ns = wide.shape[1]
    lanes = BLOCKS * m
    lane_bits, part_bits = lanes.bit_length() - 1, m.bit_length() - 1
    dq = depth // QUARTERS
    per = QUARTERS // (m // n)
    nb2 = sg_in.shape[-2]
    total = BLOCKS * chunks
    last = n - 1
    dcw = depth // m

    barrier = pltpu.get_barrier_semaphore()
    for d in range(1, m):
        pl.semaphore_signal(barrier, inc=1, device_id={"tp": lax.rem(t + d, m)}, device_id_type=MESH)
    for d in range(1, n):
        pl.semaphore_signal(barrier, inc=1, device_id={"fsdp": lax.rem(f + d, n)}, device_id_type=MESH)

    def base_copy(c, slot, which, src):
        return pltpu.make_async_copy(
            src.at[pl.ds(al(f * depth, 16), depth), pl.ds(al(c * cw, 128), cw)],
            base.at[slot, which], b_sem.at[slot, which])

    def base_start(c, slot):
        base_copy(c, slot, 0, bg_in).start()
        base_copy(c, slot, 1, bu_in).start()

    mine = pl.ds(al(t * kr, 16), kr)
    cols = pl.ds(al(t * units, 128), units)
    local = [pltpu.make_async_copy(cg_in.at[:, cols], cg.at[mine, :], l_sem.at[0]),
             pltpu.make_async_copy(cu_in.at[:, cols], cu.at[mine, :], l_sem.at[1]),
             pltpu.make_async_copy(bd_in.at[:, pl.ds(al(f * depth, 128), depth)], bd, l_sem.at[2])]
    if here:
        local += [pltpu.make_async_copy(
            cd_in.at[pl.ds(al(t * units, 16), units), :], cd.at[:, pl.ds(al(t * dcw, 128), dcw)], l_sem.at[3]),
            pltpu.make_async_copy(sd_in.at[t], sd.at[:, pl.ds(al(t * dcw, 128), dcw)], l_sem.at[4]),
            pltpu.make_async_copy(sg_in.at[t], sct.at[0:nb2, pl.ds(al(t * kr, 128), kr)], l_sem.at[5])]
    else:
        local += [pltpu.make_async_copy(cd_in, cd, l_sem.at[3]), pltpu.make_async_copy(sd_in, sd, l_sem.at[4]),
                  pltpu.make_async_copy(sg_in, sct.at[0:nb2, :], l_sem.at[5])]
    base_start(0, 0)
    if nb2 < sct.shape[0]:
        sct[nb2:, :] = jnp.zeros_like(sct[nb2:, :])
    for copy in local:
        copy.start()

    def to_tp(b, stage, d, src, dst):
        return pltpu.make_async_remote_copy(
            src_ref=src, dst_ref=dst, send_sem=s_tp.at[stage, b, d], recv_sem=r_tp.at[stage, b, d],
            device_id={"tp": lax.rem(t + d, m)}, device_id_type=MESH)

    def to_fs(b, stage, d, src, dst):
        return pltpu.make_async_remote_copy(
            src_ref=src, dst_ref=dst, send_sem=s_fs.at[stage, b, d], recv_sem=r_fs.at[stage, b, d],
            device_id={"fsdp": lax.rem(f + d, n)}, device_id_type=MESH)

    my_feat = pl.ds(al(t * feat, 128), feat)
    my_depth = pl.ds(al(f * depth, 128), depth)

    def my_part(b):
        return pl.ds(al(b * rows + t * rp, 16), rp)

    def home_rows(part, b):
        return pl.ds(al((part * BLOCKS + b) * ns, 16), ns)

    def rows_out(b, d):
        return to_tp(b, 0, d, sent.at[home_rows(lax.rem(t + d, m), b), :], wide.at[b, :, my_feat])

    def normed_out(b, d):
        return to_fs(b, 0, d, cut.at[b, lax.rem(f + d, n)], grp.at[b, pl.ds(al(f * ns, 16), ns), :])

    def flip(bits):
        peer, bit = t, 1
        while bit <= bits:
            if bits & bit:
                peer = peer + bit - 2 * bit * lax.rem(t // bit, 2)
            bit *= 2
        return peer

    def x_copy(b, h, mask, bit):
        spot = x_ref.at[pl.ds(al(b * rows + flip(mask) * rp + h * (rp // 2), 16), rp // 2), :]
        return pltpu.make_async_remote_copy(
            src_ref=spot, dst_ref=spot, send_sem=s_x.at[b, h, mask ^ bit], recv_sem=r_x.at[b, h, mask ^ bit],
            device_id={"tp": flip(bit)}, device_id_type=MESH)

    def x_arrived(b, h, mask):
        spot = x_ref.at[pl.ds(al(b * rows + flip(mask) * rp + h * (rp // 2), 16), rp // 2), :]
        pltpu.make_async_remote_copy(
            src_ref=spot, dst_ref=spot, send_sem=s_x.at[b, h, mask], recv_sem=r_x.at[b, h, mask],
            device_id={"tp": flip(1)}, device_id_type=MESH).wait_recv()

    far_bits = [2 ** i for i in range(1, m.bit_length() - 1)]
    far_masks = sorted(range(2, m, 2), key=lambda mask: (bin(mask).count("1"), mask))
    orders = (far_bits, far_bits[::-1])

    def onward(h, mask):
        order = orders[h]
        used = [i for i, bit in enumerate(order) if mask & bit]
        return order[max(used, default=-1) + 1:]

    def relay(b, phase):
        for mask in [0] + far_masks:
            if bin(mask).count("1") == phase:
                for h in range(2):
                    if mask:
                        x_arrived(b, h, mask)
                    for bit in onward(h, mask) + [1]:
                        x_copy(b, h, mask, bit).start()

    def x_wait(b):
        for mask in range(1, m, 2):
            for h in range(2):
                x_arrived(b, h, mask)

    def x_sent(b):
        for mask in [0] + far_masks:
            for h in range(2):
                for bit in onward(h, mask) + [1]:
                    x_copy(b, h, mask, bit).wait_send()

    def sum_out(b, q, d):
        return pltpu.make_async_remote_copy(
            src_ref=part_out.at[b, q, pl.ds(al(lax.rem(t + d, m) * rp, 16), rp), :], dst_ref=part_in.at[b, q, t],
            send_sem=s_sum.at[b, q, d], recv_sem=r_sum.at[b, q, d],
            device_id={"tp": lax.rem(t + d, m)}, device_id_type=MESH)

    def quarter(q):
        return pl.ds(al(f * depth + q * dq, 128), dq)

    def back_out(b, q, d):
        return pltpu.make_async_remote_copy(
            src_ref=back.at[b, q, lax.rem(f + d, n)], dst_ref=back_wide.at[b, :, quarter(q)],
            send_sem=s_back.at[b, q, d], recv_sem=r_back.at[b, q, d],
            device_id={"fsdp": lax.rem(f + d, n)}, device_id_type=MESH)

    def home_out(b, d):
        return to_tp(b, 1, d, back_wide.at[b, :, pl.ds(al(lax.rem(t + d, m) * feat, 128), feat)],
                     home.at[home_rows(t, b), :])

    def bound_copy(d):
        return pltpu.make_async_remote_copy(
            src_ref=cu_ref, dst_ref=bounds.at[f], send_sem=s_bound.at[d], recv_sem=r_bound.at[d],
            device_id={"fsdp": lax.rem(f + d, n)}, device_id_type=MESH)

    def group_counts():
        counts = [bounds[g][:, SEQS:SEQS + 1] for g in range(n)]
        starts = [jnp.zeros_like(counts[0])]
        for g in range(1, n):
            starts.append(starts[-1] + counts[g - 1])
        return starts, counts

    def home_index(axis):
        starts, counts = group_counts()
        start = sum(jnp.where(f == g, starts[g], 0) for g in range(n))
        live = sum(jnp.where(f == g, counts[g], 0) for g in range(n))
        shape = (cap, 1) if axis == 0 else (1, cap)
        r = lax.broadcasted_iota(jnp.int32, shape, axis)
        lane = (r + start) & (lanes - 1)
        index = ((lane & (m - 1)) * BLOCKS + (lane >> part_bits)) * ns + (r >> lane_bits)
        return jnp.where(r < live, index, -1)

    def slot_index(b, g, axis):
        starts, counts = group_counts()
        shape = (ns, 1) if axis == 0 else (1, ns)
        r = ((t + m * b - starts[g]) & (lanes - 1)) + lanes * lax.broadcasted_iota(jnp.int32, shape, axis)
        return jnp.where(r < counts[g], (starts[g] + r) >> lane_bits, -1)

    def ones_at(mask):
        return jnp.where(mask, 1.0, 0.0).astype(BF16)

    def scale_copy(d):
        to = lax.rem(t + d, m)
        return pltpu.make_async_remote_copy(
            src_ref=sg_in.at[to], dst_ref=sct.at[0:nb2, pl.ds(al(t * kr, 128), kr)],
            send_sem=s_sc.at[0, d], recv_sem=r_sc.at[0, d], device_id={"tp": to}, device_id_type=MESH)

    def scale_down_copy(d):
        to = lax.rem(t + d, m)
        return pltpu.make_async_remote_copy(
            src_ref=sd_in.at[to], dst_ref=sd.at[:, pl.ds(al(t * dcw, 128), dcw)],
            send_sem=s_sc.at[1, d], recv_sem=r_sc.at[1, d], device_id={"tp": to}, device_id_type=MESH)

    def code_copy(c, which, d):
        src, dst = ((cg_in, cg), (cu_in, cu))[which]
        to = lax.rem(t + d, m)
        return pltpu.make_async_remote_copy(
            src_ref=src.at[:, pl.ds(al(to * units + c * cw, 128), cw)],
            dst_ref=dst.at[mine, pl.ds(al(c * cw, 128), cw)],
            send_sem=s_code.at[c, which, d], recv_sem=r_code.at[c, which, d],
            device_id={"tp": to}, device_id_type=MESH)

    def down_copy(d):
        to = lax.rem(t + d, m)
        return pltpu.make_async_remote_copy(
            src_ref=cd_in.at[pl.ds(al(to * units, 16), units), :],
            dst_ref=cd.at[:, pl.ds(al(t * dcw, 128), dcw)],
            send_sem=s_down.at[d], recv_sem=r_down.at[d],
            device_id={"tp": to}, device_id_type=MESH)

    def codes_start(c):
        for d in range(1, m):
            code_copy(c, 0, d).start()
            code_copy(c, 1, d).start()

    def normalise(b):
        for d in range(1, m):
            rows_out(b, d).wait_recv()
        values = wide[b].astype(F32)
        inverse = lax.rsqrt(jnp.mean(values * values, axis=1, keepdims=True) + EPSILON)
        normed = (values * inverse * gain_ref[...]).astype(BF16)
        for j in range(n):
            cut[b, j] = normed[:, j * depth:(j + 1) * depth]
        grp[b, pl.ds(al(f * ns, 16), ns), :] = cut[b, f]
        for d in range(1, n):
            normed_out(b, d).start()

    def gather(b):
        for d in range(1, n):
            normed_out(b, d).wait_recv()
        mine_x = jnp.zeros((rp, depth), F32)
        for g in range(n):
            place = ones_at(lax.broadcasted_iota(jnp.int32, (rp, ns), 0) == slot_index(b, g, 1))
            mine_x = mine_x + jnp.dot(place, grp[b, g * ns:(g + 1) * ns, :], preferred_element_type=F32)
        x_ref[my_part(b), :] = mine_x.astype(BF16)
        relay(b, 0)

    pl.semaphore_wait(barrier, m + n - 2)
    for d in range(1, n):
        bound_copy(d).start()
    bounds[f] = cu_ref[...]
    for d in range(1, n):
        bound_copy(d).wait_recv()
    place_of = home_index(1)
    step = 2 * BLOCKS * ns
    for i in range(m // 2):
        spread = ones_at(lax.broadcasted_iota(jnp.int32, (step, cap), 0) + i * step == place_of)
        sent[i * step:(i + 1) * step, :] = jnp.dot(spread, tok_ref[...], preferred_element_type=F32).astype(BF16)
    for b in range(BLOCKS):
        for d in range(1, m):
            rows_out(b, d).start()
    if here:
        for d in range(1, m):
            scale_copy(d).start()
            scale_down_copy(d).start()
    codes_start(0)
    for b in range(BLOCKS):
        wide[b, :, my_feat] = sent[home_rows(t, b), :]
    normalise(0)
    gather(0)
    local[5].wait()
    if here:
        for d in range(1, m):
            scale_copy(d).wait_recv()
    for j in range(depth // 128):
        st[j * 128:(j + 1) * 128, :] = sct[:, j * 128:(j + 1) * 128].T
    for phase in range(1, len(far_bits) + 1):
        relay(0, phase)
    ahead = min(3, chunks)
    for c in range(1, ahead):
        codes_start(c)
    local[0].wait()
    local[1].wait()

    def unpack(c):
        slot = lax.rem(c, 2)

        @pl.when(c + 1 < chunks)
        def _():
            base_start(c + 1, 1 - slot)
        base_copy(c, slot, 0, bg_in).wait()
        base_copy(c, slot, 1, bu_in).wait()
        for d in range(1, m):
            code_copy(c, 0, d).wait_recv()
            code_copy(c, 1, d).wait_recv()
        there = pl.ds(al(c * cw, 128), cw)
        scales = st[...]
        lane = lax.broadcasted_iota(jnp.int32, scales.shape, 1)
        for which, codes in ((0, cg), (1, cu)):
            picked = jnp.where(lane == c + which * chunks, scales, 0.0)
            column = jnp.sum(picked, axis=1, keepdims=True)
            codes[:, there] = (base[slot, which].astype(F32) + codes[:, there].astype(F32) * column).astype(BF16)

    def partial(k):
        b, c = k // chunks, lax.rem(k, chunks)

        @pl.when(c == 0)
        def _():
            x_wait(b)

        @pl.when(b == 0)
        def _():
            unpack(c)
        there = pl.ds(al(c * cw, 128), cw)
        both = jnp.concatenate([cg[:, there], cu[:, there]], axis=1)
        for side in range(2):
            xs = x_ref[pl.ds(al(b * rows + side * half, 16), half), :]
            own[side, k] = jnp.dot(xs, both, preferred_element_type=F32).astype(BF16)

    piece = half // SUB

    def spot(k, side, u):
        b, c = k // chunks, lax.rem(k, chunks)
        return hid.at[pl.ds(al(b * rows + side * half + u * piece, 16), piece), pl.ds(al(c * cw, 128), cw)]

    def red_copy(k, side, u):
        there = pl.ds(u * piece, piece)
        return pltpu.make_async_remote_copy(
            src_ref=own.at[side, k, there, :], dst_ref=got.at[side, k, there, :],
            send_sem=s_red.at[side, k, u], recv_sem=r_red.at[side, k, u],
            device_id={"fsdp": jnp.clip(f + (1 if side else -1), 0, last)}, device_id_type=MESH)

    def hid_copy(k, side, u):
        return pltpu.make_async_remote_copy(
            src_ref=spot(k, side, u), dst_ref=spot(k, side, u),
            send_sem=s_hid.at[side, k, u], recv_sem=r_hid.at[side, k, u],
            device_id={"fsdp": jnp.clip(f + (-1 if side else 1), 0, last)}, device_id_type=MESH)

    def valid(k):
        return (k >= 0) & (k < total)

    def reduce_step(s, side, u):
        far = f if side else last - f
        k = s - far
        there = pl.ds(u * piece, piece)

        @pl.when(valid(k) & (far > 0))
        def _():
            red_copy(k, side, u).wait_recv()

            @pl.when(far < last)
            def _():
                own[side, k, there] = (own[side, k, there].astype(F32) + got[side, k, there].astype(F32)).astype(BF16)

            @pl.when(far == last)
            def _():
                both = own[side, k, there].astype(F32) + got[side, k, there].astype(F32)
                gate, up = both[:, :cw], both[:, cw:]
                b, c = k // chunks, lax.rem(k, chunks)
                hid[pl.ds(al(b * rows + side * half + u * piece, 16), piece), pl.ds(al(c * cw, 128), cw)] = (
                    jax.nn.silu(gate) * up).astype(BF16)

    def reduce_send(s, side, u):
        far = f if side else last - f
        k = s - far

        @pl.when(valid(k) & (far < last))
        def _():
            red_copy(k, side, u).start()

        @pl.when(valid(k) & (far == last))
        def _():
            hid_copy(k, side, u).start()

    def pass_on(s, side, u):
        far = f if side else last - f
        k = s - last - (last - far)

        @pl.when(valid(k) & (far < last))
        def _():
            hid_copy(k, side, u).wait_recv()

            @pl.when(far > 0)
            def _():
                hid_copy(k, side, u).start()

    def down_weights():
        for i in range(2, 5):
            local[i].wait()
        if here:
            for d in range(1, m):
                scale_down_copy(d).wait_recv()
                down_copy(d).wait_recv()

        @pl.loop(0, chunks)
        def _(c):
            there = pl.ds(al(c * cw, 16), cw)
            cd[there, :] = (bd[there, :].astype(F32) + cd[there, :].astype(F32) * sd[pl.ds(c, 1), :]).astype(BF16)

    def down(b):
        for q in range(QUARTERS):
            block = jnp.dot(hid[pl.ds(al(b * rows, 16), rows), :], cd[:, q * dq:(q + 1) * dq],
                            preferred_element_type=F32)
            part_out[b, q] = block.astype(BF16)
            for d in range(1, m):
                sum_out(b, q, d).start()

    def send_back(b, q):
        acc = part_out[b, q, pl.ds(al(t * rp, 16), rp), :].astype(F32)
        for d in range(1, m):
            sum_out(b, q, d).wait_recv()
        for d in range(1, m):
            acc = acc + part_in[b, q, lax.rem(t + d, m)].astype(F32)
        acc = acc.astype(BF16)
        for g in range(n):
            place = ones_at(lax.broadcasted_iota(jnp.int32, (ns, rp), 1) == slot_index(b, g, 0))
            back[b, q, g] = jnp.dot(place, acc, preferred_element_type=F32).astype(BF16)
        for d in range(1, n):
            back_out(b, q, d).start()
        back_wide[b, :, quarter(q)] = back[b, q, f]

    def send_home(b, h):
        for q in range(h * per, (h + 1) * per):
            for d in range(1, n):
                back_out(b, q, d).wait_recv()
        for d in range(1, m):
            @pl.when(lax.rem(lax.rem(t + d, m), m // n) == h)
            def _():
                home_out(b, d).start()

        @pl.when(lax.rem(t, m // n) == h)
        def _():
            home[home_rows(t, b), :] = back_wide[b, :, my_feat]

    def drain():
        @pl.loop(0, chunks)
        def _(c):
            for d in range(1, m):
                code_copy(c, 0, d).wait_send()
                code_copy(c, 1, d).wait_send()
        if here:
            for d in range(1, m):
                down_copy(d).wait_send()
                scale_copy(d).wait_send()
                scale_down_copy(d).wait_send()
        for b in range(BLOCKS):
            for d in range(1, m):
                rows_out(b, d).wait_send()
            x_sent(b)
            for d in range(1, n):
                normed_out(b, d).wait_send()

        for d in range(1, n):
            bound_copy(d).wait_send()

        @pl.loop(0, total)
        def _(k):
            for side in range(2):
                far = f if side else last - f

                @pl.when(far < last)
                def _():
                    for u in range(SUB):
                        red_copy(k, side, u).wait_send()

                @pl.when(far > 0)
                def _():
                    for u in range(SUB):
                        hid_copy(k, side, u).wait_send()

    steps = total + 2 * last
    tasks = [(chunks - 1 + 2 * last, down_weights)]
    for b in range(1, BLOCKS):
        tasks.append((0, functools.partial(normalise, b)))
        tasks.append((3, functools.partial(gather, b)))
        for phase in range(1, len(far_bits) + 1):
            tasks.append((3 + 2 * phase, functools.partial(relay, b, phase)))
    if here:
        for d in range(1, m):
            tasks.append((max(chunks - 3, 0) + d, down_copy(d).start))
    for b in range(BLOCKS):
        at = (b + 1) * chunks - 1 + 2 * last
        tasks.append((at, functools.partial(down, b)))
        for q in range(QUARTERS):
            tasks.append((at + 3 + q // 2, functools.partial(send_back, b, q)))
            if q % per == per - 1:
                tasks.append((at + 5 + q // 2, functools.partial(send_home, b, q // per)))

    partial(0)

    @pl.loop(0, steps)
    def _(s):
        for u in range(SUB):
            for side in range(2):
                reduce_step(s, side, u)
            for side in range(2):
                reduce_send(s, side, u)
        for u in range(SUB):
            for side in range(2):
                pass_on(s, side, u)

        @pl.when(s + ahead < chunks)
        def _():
            codes_start(s + ahead)

        @pl.when(s + 1 < total)
        def _():
            partial(s + 1)
        for at, task in tasks:
            if at < steps:
                pl.when(s == at)(task)

    late = [task for at, task in tasks if at >= steps]
    for task in [drain] + late:
        task()
    for b in range(BLOCKS):
        for d in range(1, m):
            home_out(b, d).wait_recv()
    place_of = home_index(0)
    for i in range(0, cap, 256):
        stop = min(i + 256, cap)
        spread = ones_at(lax.broadcasted_iota(jnp.int32, (stop - i, m * BLOCKS * ns), 1) == place_of[i:stop])
        summed = jnp.dot(spread, home[...], preferred_element_type=F32)
        mixed = (tok_ref[i:stop, :].astype(F32) + summed).astype(BF16).astype(F32)
        out_ref[i:stop, :] = jnp.where(place_of[i:stop] >= 0, mixed, 0.0).astype(BF16)
    seq = lax.broadcasted_iota(jnp.int32, (SEQS, 1), 0)
    low = sum(jnp.where(seq == j, cu_ref[:, j:j + 1], 0) for j in range(SEQS))
    high = sum(jnp.where(seq == j, cu_ref[:, j + 1:j + 2], 0) for j in range(SEQS))
    row = lax.broadcasted_iota(jnp.int32, (SEQS, cap), 1)
    member = ones_at((row >= low) & (row < high))
    mean_ref[...] = jnp.dot(member, out_ref[...], preferred_element_type=F32) / (high - low).astype(F32)

    for b in range(BLOCKS):
        for d in range(1, m):
            home_out(b, d).wait_send()
            for q in range(QUARTERS):
                sum_out(b, q, d).wait_send()
        for d in range(1, n):
            for q in range(QUARTERS):
                back_out(b, q, d).wait_send()


def layer(n, m, here, tokens, gain, cu_seqlens, code_gate, code_up, scales, base_gate, base_up,
          code_down, scale_down, base_down):
    width, units = base_gate.shape
    depth = width // n
    cap, feat = tokens.shape
    live_all = n * (cap // 2 + SEQS)
    ns = -(-(-(-cap // (BLOCKS * m))) // 16) * 16
    chunks = scale_down.shape[-2]
    cw = units // chunks
    total = BLOCKS * chunks
    half = live_all // (2 * BLOCKS)
    rp = live_all // (BLOCKS * m)
    dq = depth // QUARTERS
    anywhere = pl.BlockSpec(memory_space=pl.ANY)
    near = pl.BlockSpec(memory_space=pltpu.VMEM)
    dma = pltpu.SemaphoreType.DMA
    vm = pltpu.VMEM
    return pl.pallas_call(
        functools.partial(layer_kernel, n, m, here),
        out_shape=(jax.ShapeDtypeStruct((cap, feat), BF16), jax.ShapeDtypeStruct((SEQS, feat), F32)),
        in_specs=[near, near, near] + [anywhere] * 8,
        out_specs=(near, near),
        scratch_shapes=[
            vm((depth, units), BF16), vm((depth, units), BF16), vm((2, 2, depth, cw), BF16),
            vm((2, total, half, 2 * cw), BF16), vm((2, total, half, 2 * cw), BF16),
            vm((live_all, units), BF16), vm((units, depth), BF16), vm((units, depth), BF16),
            vm((live_all, depth), BF16), vm((BLOCKS, ns, width), BF16), vm((BLOCKS, n, ns, depth), BF16),
            vm((BLOCKS, n * ns, depth), BF16), vm((BLOCKS, QUARTERS, m * rp, dq), BF16),
            vm((BLOCKS, QUARTERS, m, rp, dq), BF16), vm((BLOCKS, QUARTERS, n, ns, dq), BF16),
            vm((BLOCKS, ns, width), BF16),
            vm((depth, 128), F32), vm((128, depth), F32), vm((chunks, depth), F32),
            vm((m * BLOCKS * ns, feat), BF16), vm((m * BLOCKS * ns, feat), BF16), vm((n,) + cu_seqlens.shape, jnp.int32),
            dma((chunks, 2, m)), dma((chunks, 2, m)), dma((m,)), dma((m,)), dma((6,)), dma((2, 2)),
            dma((2, total, SUB)), dma((2, total, SUB)), dma((2, total, SUB)), dma((2, total, SUB)),
            dma((BLOCKS, 2, m)), dma((BLOCKS, 2, m)),
            dma((2, BLOCKS, m)), dma((2, BLOCKS, m)), dma((1, BLOCKS, n)), dma((1, BLOCKS, n)), dma((2, m)), dma((2, m)),
            dma((BLOCKS, QUARTERS, m)), dma((BLOCKS, QUARTERS, m)), dma((BLOCKS, QUARTERS, n)), dma((BLOCKS, QUARTERS, n)),
            dma((n,)), dma((n,)),
        ],
        compiler_params=pltpu.CompilerParams(
            collective_id=0, has_side_effects=True, vmem_limit_bytes=67043328),
    )(tokens, gain, cu_seqlens, code_gate, code_up, scales, base_gate, base_up, code_down, scale_down, base_down)


def shards(tokens, norm_gain, base_gate, base_up, base_down, code_gate, code_up,
           scale_gate, scale_up, code_down, scale_down, cu_seqlens):
    n, m = lax.axis_size("fsdp"), lax.axis_size("tp")
    kr = code_gate.shape[0]
    nb = scale_gate.shape[1] // m
    scales = jnp.concatenate([scale_gate.reshape(kr, m, nb), scale_up.reshape(kr, m, nb)], axis=2).transpose(1, 2, 0)
    scales = jnp.pad(scales, ((0, 0), (0, -(2 * nb) % 8), (0, 0)))
    scale_down = scale_down.reshape(m, nb, -1)
    here = code_down.shape[1] % 128 == 0 and kr % 128 == 0
    if not here:
        code_down = lax.all_to_all(code_down, "tp", split_axis=0, concat_axis=1, tiled=True)
        scales = lax.all_to_all(scales, "tp", split_axis=0, concat_axis=2, tiled=True)[0]
        scale_down = lax.all_to_all(scale_down, "tp", split_axis=0, concat_axis=2, tiled=True)[0]
    return layer(n, m, here, tokens, norm_gain[None, :], cu_seqlens, code_gate, code_up, scales,
                 base_gate, base_up, code_down, scale_down, base_down)


def solution(mesh):
    placed = (
        P("fsdp", "tp"), P(), P(None, "tp"), P(None, "tp"), P("tp", None),
        P(("fsdp", "tp"), None), P(("fsdp", "tp"), None),
        P(("fsdp", "tp"), None), P(("fsdp", "tp"), None),
        P(None, ("fsdp", "tp")), P(None, ("fsdp", "tp")), P("fsdp", None),
    )
    return jax.shard_map(shards, mesh=mesh, in_specs=placed,
                         out_specs=(P("fsdp", "tp"), P("fsdp", "tp")), check_vma=False)
```
